32 devices in a mesh: dp: 2 (over x), fsdp: 16 (over z, y, core).
Axes of the slice: x: 2, y: 2, z: 4, core: 2. Of those that a mesh axis runs over, the one named last changes fastest.
Arguments:
- hidden: bfloat16 [16384, 512], P(('dp', 'fsdp')), parts along dimension 0
- targets: int32 [16384], P(('dp', 'fsdp')), parts along dimension 0
- weight: bfloat16 [32128, 512], P('fsdp')
Outputs:
- output 1: float32 [2], P('dp'), parts along dimension 0
- output 2: float32 [16384, 512], P(('dp', 'fsdp')), parts along dimension 0
- output 3: float32 [64256, 512], P(('dp', 'fsdp')), parts along dimension 0
There are 2 independent parts. The reference program is written for one: setup_inputs(seed, part) draws one part's arguments, and reference() takes and returns one part's arrays. A program takes and returns all parts, laid end to end along the dimension named above; an argument that names none is the same for every part.
All inputs are finite; a program needn't handle non-finite values.
Results may differ from the reference program's by a relative error of at most 0.001.
Values are sent between devices in bfloat16 or wider.
A program may use at most 1 GiB of HBM per device.

```python
import jax
import jax.numpy as jnp
from jax import lax

TOKENS = 8192
VOCAB = 32128
WIDTH = 512
BLOCKS = 16

BLOCK_ROWS = VOCAB // BLOCKS


def setup_inputs(seed: int = 0, part: int = 0) -> dict:
    base_key = jax.random.key(seed)
    key_hid, key_tgt, key_wgt = jax.random.split(base_key, 3)
    key_hid = jax.random.fold_in(key_hid, part)
    key_tgt = jax.random.fold_in(key_tgt, part)
    hidden = jax.random.normal(key_hid, (TOKENS, WIDTH), jnp.float32).astype(jnp.bfloat16)
    targets = jax.random.randint(key_tgt, (TOKENS,), 0, VOCAB, dtype=jnp.int32)
    weight = (jax.random.normal(key_wgt, (VOCAB, WIDTH), jnp.float32) * WIDTH ** -0.5).astype(jnp.bfloat16)
    return {"hidden": hidden, "targets": targets, "weight": weight}


def reference(hidden, targets, weight):
    w_blocks = weight.reshape(BLOCKS, BLOCK_ROWS, WIDTH)
    blk_starts = jnp.arange(BLOCKS, dtype=jnp.int32) * BLOCK_ROWS
    col_ids = jnp.arange(BLOCK_ROWS, dtype=jnp.int32)

    def block_logits(w_blk, blk_start):
        logits = jnp.dot(hidden, w_blk.T, preferred_element_type=jnp.float32)
        is_target = (targets - blk_start)[:, None] == col_ids[None, :]
        return logits, is_target

    def fwd_step(fwd_state, blk_pair):
        run_max, run_sum, tgt_logit = fwd_state
        logits, is_target = block_logits(blk_pair[0], blk_pair[1])
        new_max = jnp.maximum(run_max, jnp.max(logits, axis=1))
        run_sum = run_sum * jnp.exp(run_max - new_max) + jnp.sum(jnp.exp(logits - new_max[:, None]), axis=1)
        tgt_logit = tgt_logit + jnp.sum(jnp.where(is_target, logits, 0.0), axis=1)
        return (new_max, run_sum, tgt_logit), None

    init_state = (jnp.full((TOKENS,), -jnp.inf, jnp.float32), jnp.zeros((TOKENS,), jnp.float32), jnp.zeros((TOKENS,), jnp.float32))
    run_max, run_sum, tgt_logit = lax.scan(fwd_step, init_state, (w_blocks, blk_starts))[0]
    log_norm = run_max + jnp.log(run_sum)
    loss_val = (jnp.sum(log_norm - tgt_logit) / TOKENS).reshape(1)

    def bwd_step(dh_acc, blk_pair):
        logits, is_target = block_logits(blk_pair[0], blk_pair[1])
        dlogits = ((jnp.exp(logits - log_norm[:, None]) - is_target.astype(jnp.float32)) / TOKENS).astype(jnp.bfloat16)
        dh_acc = dh_acc + jnp.dot(dlogits, blk_pair[0], preferred_element_type=jnp.float32)
        dw_blk = jnp.dot(dlogits.T, hidden, preferred_element_type=jnp.float32)
        return dh_acc, dw_blk

    grad_hidden, dw_blocks = lax.scan(bwd_step, jnp.zeros((TOKENS, WIDTH), jnp.float32), (w_blocks, blk_starts))
    return loss_val, grad_hidden, dw_blocks.reshape(VOCAB, WIDTH)
```

```python
import jax
import jax.numpy as jnp
from jax import lax
from jax.sharding import PartitionSpec as P


def solution(mesh):
    groups = mesh.shape["fsdp"]
    tok_spec = P(("dp", "fsdp"), None)

    def local_head(hidden, targets, weight):
        tokens = hidden.shape[0] * groups
        rows = weight.shape[0]
        base = lax.axis_index("fsdp") * rows
        h_all = lax.all_gather(hidden, "fsdp", axis=0, tiled=True)
        t_all = lax.all_gather(targets, "fsdp", axis=0, tiled=True)
        logits = lax.dot_general(h_all, weight, (((1,), (1,)), ((), ())), preferred_element_type=jnp.float32)
        is_target = (t_all - base)[:, None] == jnp.arange(rows, dtype=jnp.int32)[None, :]
        row_max = jnp.max(logits, axis=1)
        row_sum = jnp.sum(jnp.exp(logits - row_max[:, None]), axis=1)
        tgt = jnp.sum(jnp.where(is_target, logits, 0.0), axis=1)
        stats = lax.all_gather(jnp.stack([row_max, row_sum, tgt]), "fsdp", axis=0)
        all_max = jnp.max(stats[:, 0], axis=0)
        lse = all_max + jnp.log(jnp.sum(stats[:, 1] * jnp.exp(stats[:, 0] - all_max), axis=0))
        loss = (jnp.sum(lse - jnp.sum(stats[:, 2], axis=0)) / tokens).reshape(1)
        dz = ((jnp.exp(logits - lse[:, None]) - is_target.astype(jnp.float32)) / tokens).astype(jnp.bfloat16)
        dh = jnp.dot(dz, weight, preferred_element_type=jnp.float32)
        dh = lax.psum_scatter(dh, "fsdp", scatter_dimension=0, tiled=True)
        dw = lax.dot_general(dz, h_all, (((0,), (0,)), ((), ())), preferred_element_type=jnp.float32)
        return loss, dh, dw

    return jax.shard_map(local_head, mesh=mesh, in_specs=(tok_spec, P(("dp", "fsdp")), P("fsdp", None)), out_specs=(P("dp"), tok_spec, tok_spec), check_vma=False)
```

```python
import functools

import jax
import jax.numpy as jnp
from jax import lax
from jax.experimental import pallas as pl
from jax.experimental.pallas import tpu as pltpu
from jax.sharding import PartitionSpec as P

MESH = pl.DeviceIdType.MESH
BF16, F32 = jnp.bfloat16, jnp.float32
COLUMN = ((1, 2, 3), (2, 0, 3), (1, 3, 0), (2, 1, 0))
DESTS = ((3, 2, 1, 0), (3, 0, 2, 1), (0, 3, 1, 2), (0, 1, 2, 3))
PIECES = 4
SCHEDULE = (
    ("far", 0), ("near", 0), ("far", 1), ("hop", 0, 0), ("hop", 0, 1), ("near", 1), ("hop", 0, 2), ("hop", 0, 3),
    ("far", 2), ("hop", 1, 0), ("near", 2), ("hop", 1, 1), ("hop", 1, 2), ("far", 3), ("hop", 1, 3), ("hop", 2, 0),
    ("near", 3), ("dw_send",), ("hop", 2, 1), ("hop", 2, 2), ("hop", 2, 3), ("hop", 3, 0), ("dw_add",),
    ("hop", 3, 1), ("hop", 3, 2), ("hop", 3, 3),
)


def pick(z, table):
    lo, hi = z % 2, z // 2
    return table[0] * (1 - lo) * (1 - hi) + table[1] * lo * (1 - hi) + table[2] * (1 - lo) * hi + table[3] * lo * hi


def head_kernel(vocab, tile, h_ref, t_ref, w_ref, loss_ref, dht_ref, dw_out, x_all, xt_all, t_all, w_all, wt_all, dw, dw_in,
                far, near, far_in, chain, stats, lse, zt_row, loss_rows,
                x_recv, x_send, t_recv, t_send, w_sem, st_recv, st_send, ls_recv, ls_send, y_send, y_recv, c_send, c_recv,
                dw_sem, out_sem):
    tb, d = h_ref.shape
    vp = w_all.shape[0] // 2
    nt = vp // tile
    groups = tile // 8
    live = (vocab - (nt - 1) * tile) // 8
    qd = d // PIECES
    r = lax.axis_index("fsdp")
    c, chip = r % 2, r // 2
    y, z = chip % 2, chip // 2
    mate, across, left, right = r + 1 - 2 * c, r + 2 - 4 * y, r - 4, r + 4

    def remote(src, dst, ss, rs, dev):
        return pltpu.make_async_remote_copy(src_ref=src, dst_ref=dst, send_sem=ss, recv_sem=rs, device_id={"fsdp": dev}, device_id_type=MESH)

    def drain(ref, sem):
        pltpu.make_async_copy(ref, ref, sem).wait()

    barrier = pltpu.get_barrier_semaphore()
    for i in range(1, 16):
        pl.semaphore_signal(barrier, inc=1, device_id={"fsdp": (r + i) % 16}, device_id_type=MESH)

    w_all[pl.ds(vp - tile, tile), :] = jnp.zeros((tile, d), BF16)
    w_all[pl.ds(0, vocab), :] = w_ref[...]

    def transpose_w(i, _):
        wt_all[i] = w_all[pl.ds(pl.multiple_of(i * tile, tile), tile), :].T
        return 0

    lax.fori_loop(0, nt, transpose_w, 0)
    x_all[chip] = h_ref[...]
    t_all[chip] = t_ref[...]
    pl.semaphore_wait(barrier, 15)

    w_copy = remote(w_all.at[pl.ds(0, vp)], w_all.at[pl.ds(vp, vp)], w_sem.at[0], w_sem.at[1], mate)
    w_copy.start()

    def x_copy(dev, b, dirn, idx):
        return remote(x_all.at[b], x_all.at[b], x_send.at[dirn, idx], x_recv.at[b], dev)

    def t_copy(i):
        return remote(t_all.at[chip], t_all.at[chip], t_send, t_recv.at[chip], (2 * chip + 2 * i) % 16 + c)

    x_copy(across, chip, 0, 3).start()

    @pl.when(z > 0)
    def _():
        x_copy(left, chip, 1, 3).start()

    @pl.when(z < 3)
    def _():
        x_copy(right, chip, 2, 3).start()

    for i in range(1, 8):
        t_copy(i).start()
    w_copy.wait()
    lax.fori_loop(nt, 2 * nt, transpose_w, 0)

    def zero_dw(i, _):
        dw[pl.ds(pl.multiple_of(i * tile, tile), tile), :] = jnp.zeros((tile, d), F32)
        return 0

    lax.fori_loop(0, 2 * nt, zero_dw, 0)

    iota8 = lax.broadcasted_iota(jnp.int32, (8, tb), 0)
    group8 = lax.broadcasted_iota(jnp.int32, (groups, 8, tb), 0) * 8

    def target_rows(b, i):
        slot = i // nt
        rel = t_all[b] - vocab * (r * (1 - slot) + mate * slot)
        rel = jnp.where((rel >= 0) & (rel < vocab), rel, -vp)
        return jnp.broadcast_to(rel - (i % nt) * tile, (8, tb)) - iota8

    def tile_logits(b, i):
        rows = pl.ds(pl.multiple_of(i * tile, tile), tile)
        return jnp.dot(w_all[rows, :], xt_all[b], preferred_element_type=F32).reshape(groups, 8, tb)

    def mask_pad(vals, i, fill):
        if live == groups:
            return vals
        tail = jnp.where((jnp.zeros((groups - live, 8, tb), jnp.int32) + i % nt) == nt - 1, fill, vals[live:])
        return jnp.concatenate([vals[:live], tail], axis=0)

    zt_row[...] = jnp.zeros_like(zt_row)

    def forward(step, codes):
        code_z, code_y = codes
        zs, flip = code_z % 4, code_y % 2
        b = 2 * zs + y + flip * (1 - 2 * y)

        @pl.when(step > 0)
        def _():
            drain(x_all.at[b], x_recv.at[b])
            drain(t_all.at[b], t_recv.at[b])

        @pl.when((step > 0) & (flip == 0))
        def _():
            k = (step - 1) // 2
            x_copy(across, b, 0, k).start()

            @pl.when((zs > z) & (z > 0))
            def _():
                x_copy(left, b, 1, k).start()

            @pl.when((zs < z) & (z < 3))
            def _():
                x_copy(right, b, 2, k).start()

        xt_all[b] = x_all[b].T

        def tile_step(i, carry):
            m, s, zt = carry
            zv = tile_logits(b, i)
            hit = target_rows(b, i)[None] == group8
            zt = zt + jnp.sum(jnp.where(hit, zv, 0.0), axis=0)
            zv = mask_pad(zv, i, -jnp.inf)
            m_new = jnp.maximum(m, jnp.max(zv, axis=0))
            s = s * jnp.exp(m - m_new) + jnp.sum(jnp.exp(zv - m_new[None]), axis=0)
            return m_new, s, zt

        zero = jnp.zeros((8, tb), F32)
        m, s, zt = lax.fori_loop(0, 2 * nt, tile_step, (jnp.full((8, tb), -jnp.inf, F32), zero, zero))
        m1 = jnp.max(m, axis=0, keepdims=True)
        s1 = jnp.sum(s * jnp.exp(m - m1), axis=0, keepdims=True)
        stats[chip, b] = jnp.concatenate([m1, s1], axis=0)
        zt_row[...] += jnp.sum(zt, axis=0, keepdims=True)
        for i in range(1, 8):
            remote(stats.at[chip, b], stats.at[chip, b], st_send, st_recv.at[chip], (2 * chip + 2 * i) % 16 + c).start()
        return code_z // 4, code_y // 2

    zlists = [(q, COLUMN[q][0], q, COLUMN[q][1], COLUMN[q][0], COLUMN[q][2], COLUMN[q][1], COLUMN[q][2]) for q in range(4)]
    code_z = pick(z, [sum(v * 4**s for s, v in enumerate(zl)) for zl in zlists])
    code_y = sum(v * 2**s for s, v in enumerate((0, 0, 1, 0, 1, 0, 1, 1)))
    lax.fori_loop(0, 8, forward, (code_z, jnp.int32(code_y)))

    for i in range(1, 8):
        src = (chip + i) % 8
        drain(stats.at[src], st_recv.at[src])

    def combine(b, _):
        ms = [stats[q, b][0:1] for q in range(8)]
        top = functools.reduce(jnp.maximum, ms)
        tot = sum(stats[q, b][1:2] * jnp.exp(ms[q] - top) for q in range(8))
        lse[b] = top + jnp.log(tot)
        return 0

    lax.fori_loop(0, 8, combine, 0)
    loss_rows[r] = lse[chip] - zt_row[...]

    def loss_copy(i):
        return remote(loss_rows.at[r], loss_rows.at[r], ls_send, ls_recv, (r + i) % 16)

    for i in range(1, 16):
        loss_copy(i).start()

    def backward(b, acc):
        acc[...] = jnp.zeros((d, tb), F32)
        norm = jnp.broadcast_to(lse[b], (8, tb))[None]

        def tile_step(i, _):
            rows = pl.ds(pl.multiple_of(i * tile, tile), tile)
            prob = jnp.exp(tile_logits(b, i) - norm)
            hit = target_rows(b, i)[None] == group8
            dz = mask_pad(prob - jnp.where(hit, 1.0, 0.0), i, 0.0)
            dz = dz.reshape(tile, tb).astype(BF16)
            acc[...] += jnp.dot(wt_all[i], dz, preferred_element_type=F32)
            dw[rows, :] += jnp.dot(dz, x_all[b], preferred_element_type=F32)
            return 0

        lax.fori_loop(0, 2 * nt, tile_step, 0)

    def dest(k):
        return pick(z, [DESTS[q][k] for q in range(4)])

    def y_copy(k, q):
        rows = pl.ds(q * qd, qd)
        return remote(far.at[k, rows], far_in.at[k, rows], y_send.at[k, q], y_recv.at[k, q], across)

    def chain_copy(k, q, slot, dev):
        rows = pl.ds(q * qd, qd)
        return remote(near.at[k, rows], chain.at[slot, rows], c_send.at[k, q], c_recv.at[slot, q], dev)

    def hop(k, q):
        zd = dest(k)
        rows = pl.ds(q * qd, qd)
        y_copy(k, q).wait_recv()
        near[k, rows] = near[k, rows] + far_in[k, rows]

        def add_chain(slot):
            drain(chain.at[slot, rows], c_recv.at[slot, q])
            near[k, rows] = near[k, rows] + chain[slot, rows]

        if k < 3:
            @pl.when(((zd > z) & (z > 0)) | ((zd < z) & (z < 3)))
            def _():
                add_chain(zd)

            @pl.when(zd > z)
            def _():
                chain_copy(k, q, zd, right).start()

            @pl.when(zd == z - 1)
            def _():
                chain_copy(k, q, 4, left).start()

            @pl.when(zd < z - 1)
            def _():
                chain_copy(k, q, zd, left).start()
        else:
            @pl.when(z > 0)
            def _():
                add_chain(z)

            @pl.when(z < 3)
            def _():
                add_chain(4)

            pltpu.make_async_copy(near.at[k, rows], dht_ref.at[rows], out_sem.at[q]).start()

    dw_copy = remote(dw.at[pl.ds(vp, vp)], dw_in, dw_sem.at[0], dw_sem.at[1], mate)
    dw_store = pltpu.make_async_copy(dw.at[pl.ds(0, vocab)], dw_out, out_sem.at[PIECES])
    for event in SCHEDULE:
        if event[0] == "far":
            backward(2 * dest(event[1]) + 1 - y, far.at[event[1]])
            for q in range(PIECES):
                y_copy(event[1], q).start()
        elif event[0] == "near":
            backward(2 * dest(event[1]) + y, near.at[event[1]])
        elif event[0] == "hop":
            hop(*event[1:])
        elif event[0] == "dw_send":
            dw_copy.start()
        else:
            dw_copy.wait_recv()

            def add_dw(i, _):
                rows = pl.ds(pl.multiple_of(i * tile, tile), tile)
                dw[rows, :] += dw_in[rows, :]
                return 0

            lax.fori_loop(0, nt, add_dw, 0)
            dw_store.start()

    drain(loss_rows.at[pl.ds(0, 15)], ls_recv)
    total = sum(loss_rows[q] for q in range(16))
    loss_ref[...] = jnp.sum(total, axis=1, keepdims=True) * jnp.ones((1, 128), F32)

    drain(loss_rows.at[pl.ds(0, 15)], ls_send)
    drain(stats.at[pl.ds(0, 7)], st_send)
    drain(t_all.at[pl.ds(0, 7)], t_send)
    x_copy(across, chip, 0, 3).wait_send()

    @pl.when(z > 0)
    def _():
        x_copy(left, chip, 1, 3).wait_send()

    @pl.when(z < 3)
    def _():
        x_copy(right, chip, 2, 3).wait_send()

    for k in range(3):
        zs = pick(z, [COLUMN[q][k] for q in range(4)])
        x_copy(across, chip, 0, k).wait_send()

        @pl.when((zs > z) & (z > 0))
        def _():
            x_copy(left, chip, 1, k).wait_send()

        @pl.when((zs < z) & (z < 3))
        def _():
            x_copy(right, chip, 2, k).wait_send()

        for q in range(PIECES):
            drain(near.at[k, pl.ds(q * qd, qd)], c_send.at[k, q])
    for k in range(4):
        for q in range(PIECES):
            y_copy(k, q).wait_send()
    dw_copy.wait_send()
    dw_store.wait()
    for q in range(PIECES):
        rows = pl.ds(q * qd, qd)
        pltpu.make_async_copy(near.at[3, rows], dht_ref.at[rows], out_sem.at[q]).wait()


def solution(mesh, tile=512):
    groups = mesh.shape["fsdp"]
    tok_spec = P(("dp", "fsdp"), None)

    def local_head(hidden, targets, weight):
        tb, d = hidden.shape
        vocab = weight.shape[0]
        vp = -(-vocab // tile) * tile
        nt = vp // tile
        dma = pltpu.SemaphoreType.DMA
        vmem = pltpu.VMEM
        loss, dht, dw = pl.pallas_call(
            functools.partial(head_kernel, vocab, tile),
            out_shape=(jax.ShapeDtypeStruct((1, 128), F32), jax.ShapeDtypeStruct((d, tb), F32), jax.ShapeDtypeStruct((vocab, d), F32)),
            in_specs=[pl.BlockSpec(memory_space=vmem)] * 3,
            out_specs=(pl.BlockSpec(memory_space=vmem), pl.BlockSpec(memory_space=pl.ANY), pl.BlockSpec(memory_space=pl.ANY)),
            scratch_shapes=[
                vmem((8, tb, d), BF16), vmem((8, d, tb), BF16), vmem((8, 1, tb), jnp.int32),
                vmem((2 * vp, d), BF16), vmem((2 * nt, d, tile), BF16),
                vmem((2 * vp, d), F32), vmem((vp, d), F32),
                vmem((4, d, tb), F32), vmem((4, d, tb), F32), vmem((4, d, tb), F32), vmem((5, d, tb), F32),
                vmem((8, 8, 2, tb), F32), vmem((8, 1, tb), F32), vmem((1, tb), F32), vmem((16, 1, tb), F32),
                dma((8,)), dma((3, 4)), dma((8,)), dma, dma((2,)), dma((8,)), dma, dma, dma,
                dma((4, PIECES)), dma((4, PIECES)), dma((3, PIECES)), dma((5, PIECES)), dma((2,)), dma((PIECES + 1,)),
            ],
            compiler_params=pltpu.CompilerParams(collective_id=0, has_side_effects=True, vmem_limit_bytes=66_000_000),
        )(hidden, targets.reshape(1, tb), weight)
        scale = 1.0 / (tb * groups)
        return loss[0, :1] * scale, dht.T * scale, dw * scale

    return jax.shard_map(local_head, mesh=mesh, in_specs=(tok_spec, P(("dp", "fsdp")), P("fsdp", None)), out_specs=(P("dp"), tok_spec, tok_spec), check_vma=False)
```

```python
import functools

import jax
import jax.numpy as jnp
from jax import lax
from jax.experimental import pallas as pl
from jax.experimental.pallas import tpu as pltpu
from jax.sharding import PartitionSpec as P

MESH = pl.DeviceIdType.MESH
BF16, F32 = jnp.bfloat16, jnp.float32
CHUNKS = 4
COLUMN = ((1, 2, 3), (2, 0, 3), (1, 3, 0), (2, 1, 0))
DESTS = ((3, 2, 1, 0), (3, 2, 0, 1), (0, 1, 3, 2), (0, 1, 2, 3))
Y_FIRST = (0, 0, 1, 1)
SCHEDULE = (
    ('A', 'own', 0), ('E', 'own', 2), ('I', 'ag', 0, 2), ('A', 'ag', 0, 0), ('E', 'own', 1), ('E', 'ag', 0, 2),
    ('I', 'own', 1), ('E', 'ag', 2, 0), ('A', 'prep', 2.5), ('I', 'ag', 0, 1), ('A', 'ag', 0, 4), ('I', 'ag', 1, 2),
    ('E', 'ag', 1, 0), ('A', 'fwd', 0, 0), ('E', 'own', 3), ('I', 'ag', 1, 0), ('I', 'own', 2), ('I', 'ag', 0, 6),
    ('I', 'ag', 1, 4), ('E', 'ag', 0, 1), ('E', 'ag', 0, 6), ('I', 'ag', 0, 5), ('E', 'ag', 0, 3), ('E', 'ag', 0, 5),
    ('I', 'ag', 0, 3), ('I', 'ag', 2, 3), ('I', 'ag', 1, 1), ('I', 'ag', 2, 1), ('A', 'fwd', 0, 1), ('E', 'ag', 1, 3),
    ('E', 'ag', 1, 4), ('I', 'ag', 2, 4), ('E', 'ag', 1, 2), ('I', 'ag', 2, 0), ('I', 'ag', 2, 6), ('A', 'stat', 0),
    ('I', 'own', 3), ('A', 'bwd', 0, 1, 0), ('E', 'ag', 2, 1), ('E', 'ag', 3, 0), ('A', 'bwd', 0, 1, 1),
    ('I', 'ag', 1, 6), ('E', 'ag', 1, 1), ('I', 'ag', 1, 3), ('I', 'ag', 1, 5), ('A', 'bwd', 0, 0, 0),
    ('I', 'ag', 2, 2), ('I', 'ag', 3, 4), ('E', 'ag', 1, 5), ('E', 'ag', 1, 6), ('A', 'fwd', 1, 1), ('I', 'ag', 3, 0),
    ('E', 'ag', 2, 2), ('A', 'fwd', 1, 0), ('I', 'ag', 3, 3), ('A', 'bwd', 0, 0, 1), ('E', 'hop', 0, 1),
    ('A', 'stat', 1), ('I', 'ag', 2, 5), ('I', 'ag', 3, 6), ('A', 'bwd', 1, 1, 0), ('E', 'ag', 2, 6),
    ('E', 'hop', 0, 0), ('A', 'bwd', 1, 1, 1), ('E', 'ag', 2, 3), ('E', 'ag', 2, 5), ('I', 'ag', 3, 1),
    ('A', 'fwd', 2, 0), ('A', 'bwd', 1, 0, 0), ('I', 'ag', 3, 2), ('E', 'ag', 3, 1), ('E', 'ag', 2, 4),
    ('I', 'ag', 3, 5), ('I', 'hop', 0, 1), ('I', 'hop', 0, 0), ('A', 'fwd', 2, 1), ('A', 'bwd', 1, 0, 1),
    ('E', 'ag', 3, 4), ('E', 'ag', 3, 6), ('A', 'stat', 2), ('E', 'hop', 1, 0), ('E', 'ag', 3, 3),
    ('A', 'bwd', 2, 1, 0), ('E', 'hop', 1, 1), ('A', 'bwd', 2, 1, 1), ('E', 'ag', 3, 5), ('A', 'bwd', 2, 0, 0),
    ('E', 'ag', 3, 2), ('E', 'hop', 1, 2), ('A', 'fwd', 3, 1), ('I', 'hop', 0, 2), ('A', 'fwd', 3, 0),
    ('I', 'hop', 1, 0), ('E', 'hop', 0, 2), ('A', 'bwd', 2, 0, 1), ('E', 'hop', 2, 0), ('I', 'hop', 1, 1),
    ('A', 'stat', 3), ('A', 'bwd', 3, 1, 0), ('A', 'bwd', 3, 0, 0), ('E', 'hop', 2, 1), ('A', 'bwd', 3, 1, 1),
    ('E', 'hop', 2, 2), ('I', 'hop', 2, 0), ('A', 'bwd', 3, 0, 1), ('A', 'dw_send'), ('I', 'hop', 1, 2),
    ('I', 'hop', 2, 1), ('A', 'hop', 3, 0), ('I', 'hop', 0, 3), ('I', 'hop', 2, 2), ('I', 'hop', 3, 1),
    ('I', 'hop', 2, 3), ('I', 'hop', 3, 2), ('E', 'hop', 1, 3), ('E', 'hop', 0, 3), ('E', 'hop', 3, 1),
    ('E', 'hop', 3, 2), ('E', 'hop', 2, 3), ('E', 'hop', 3, 3), ('A', 'dw_add'), ('I', 'hop', 1, 3),
    ('I', 'hop', 3, 3),
)


def pick(z, table):
    lo, hi = z % 2, z // 2
    return table[0] * (1 - lo) * (1 - hi) + table[1] * lo * (1 - hi) + table[2] * (1 - lo) * hi + table[3] * lo * hi


def head_kernel(vocab, tile, h_ref, t_ref, w_ref, loss_ref, dht_ref, dw_out, x_all, xt_all, t_all, w_all, wt_all, dw, dw_in,
                far, near, far_in, chain, stats, lse, zt_acc, loss_rows,
                x_recv, x_send, t_recv, t_send, w_sem, st_recv, st_send, ls_recv, ls_send, y_send, y_recv, c_send, c_recv,
                dw_sem, out_sem):
    tb, d = h_ref.shape
    tc = tb // CHUNKS
    vp = w_all.shape[0] // 2
    nt = vp // tile
    groups = tile // 8
    live = (vocab - (nt - 1) * tile) // 8
    r = lax.axis_index("fsdp")
    c, chip = r % 2, r // 2
    y, z = chip % 2, chip // 2
    mate, across, left, right = r + 1 - 2 * c, r + 2 - 4 * y, r - 4, r + 4

    def remote(src, dst, ss, rs, dev):
        return pltpu.make_async_remote_copy(src_ref=src, dst_ref=dst, send_sem=ss, recv_sem=rs, device_id={"fsdp": dev}, device_id_type=MESH)

    def drain(ref, sem):
        pltpu.make_async_copy(ref, ref, sem).wait()

    barrier = pltpu.get_barrier_semaphore()
    for i in range(1, 16):
        pl.semaphore_signal(barrier, inc=1, device_id={"fsdp": (r + i) % 16}, device_id_type=MESH)

    for k in range(CHUNKS):
        x_all[2 * k, z] = h_ref[k * tc:(k + 1) * tc, :]
    t_all[chip] = t_ref[...]
    w_all[pl.ds(vp - tile, tile), :] = jnp.zeros((tile, d), BF16)
    w_all[pl.ds(0, vocab), :] = w_ref[...]

    def transpose_w(i, _):
        wt_all[i] = w_all[pl.ds(pl.multiple_of(i * tile, tile), tile), :].T
        return 0

    def zero_dw(i, _):
        dw[pl.ds(pl.multiple_of(i * tile, tile), tile), :] = jnp.zeros((tile, d), F32)
        return 0

    lax.fori_loop(0, nt, transpose_w, 0)
    pl.semaphore_wait(barrier, 15)

    w_copy = remote(w_all.at[pl.ds(0, vp)], w_all.at[pl.ds(vp, vp)], w_sem.at[0], w_sem.at[1], mate)

    def t_copy(i):
        return remote(t_all.at[chip], t_all.at[chip], t_send, t_recv, (2 * chip + 2 * i) % 16 + c)

    def prepare():
        for i in range(1, 8):
            t_copy(i).start()
        w_copy.start()
        lax.fori_loop(0, 2 * nt, zero_dw, 0)
        zt_acc[...] = jnp.zeros_like(zt_acc)
        w_copy.wait()
        lax.fori_loop(nt, 2 * nt, transpose_w, 0)

    def x_copy(k, col, zs, way, slot):
        dev = (across, left, right)[way]
        to = 1 if way == 0 else col
        return remote(x_all.at[2 * k + col, zs], x_all.at[2 * k + to, zs], x_send.at[way, k, slot], x_recv.at[2 * k + to, zs], dev)

    def along(k, col, zs, slot, to_left, to_right, act):
        @pl.when(to_left)
        def _():
            act(x_copy(k, col, zs, 1, slot))

        @pl.when(to_right)
        def _():
            act(x_copy(k, col, zs, 2, slot))

    def own(k, act):
        act(x_copy(k, 0, z, 0, 7))
        along(k, 0, z, 7, z > 0, z < 3, act)

    def arrival(k, j):
        if Y_FIRST[k]:
            col, n = (1, 0, 1, 0, 1, 0, 1)[j], (None, 0, 0, 1, 1, 2, 2)[j]
        else:
            col, n = (0, 1, 0, 1, 0, 1, 1)[j], (0, None, 1, 0, 2, 1, 2)[j]
        return col, z if n is None else pick(z, [COLUMN[q][n] for q in range(4)])

    def relay(k, j, act):
        col, zs = arrival(k, j)
        if Y_FIRST[k]:
            along(k, col, zs, j, (zs >= z) & (z > 0), (zs <= z) & (z < 3), act)
        elif col == 0:
            act(x_copy(k, 0, zs, 0, j))
            along(k, 0, zs, j, (zs > z) & (z > 0), (zs < z) & (z < 3), act)

    def gather(k, j):
        col, zs = arrival(k, j)
        drain(x_all.at[2 * k + col, zs], x_recv.at[2 * k + col, zs])
        relay(k, j, lambda copy: copy.start())

    def tile_logits(b, i):
        rows = pl.ds(pl.multiple_of(i * tile, tile), tile)
        return jnp.dot(w_all[rows, :], xt_all[b], preferred_element_type=F32).reshape(groups, 8, tb)

    def mask_pad(vals, i, fill):
        if live == groups:
            return vals
        tail = jnp.where((jnp.zeros((groups - live, 8, tb), jnp.int32) + i % nt) == nt - 1, fill, vals[live:])
        return jnp.concatenate([vals[:live], tail], axis=0)

    def place(k, col):
        return 2 * k + y + col * (1 - 2 * y)

    def forward(k, col):
        b = 2 * k + col
        xt_all[b] = x_all[b].reshape(tb, d).T

        def tile_step(i, carry):
            m, s = carry
            zv = mask_pad(tile_logits(b, i), i, -jnp.inf)
            m_new = jnp.maximum(m, jnp.max(zv, axis=0))
            s = s * jnp.exp(m - m_new) + jnp.sum(jnp.exp(zv - m_new[None]), axis=0)
            return m_new, s

        m, s = lax.fori_loop(0, 2 * nt, tile_step, (jnp.full((8, tb), -jnp.inf, F32), jnp.zeros((8, tb), F32)))
        m1 = jnp.max(m, axis=0, keepdims=True)
        s1 = jnp.sum(s * jnp.exp(m - m1), axis=0, keepdims=True)
        p = place(k, col)
        stats[chip, p] = jnp.concatenate([m1, s1], axis=0)
        for i in range(1, 8):
            remote(stats.at[chip, p], stats.at[chip, p], st_send, st_recv.at[k], (2 * chip + 2 * i) % 16 + c).start()

    def combine(k):
        drain(stats.at[pl.ds(0, 7), pl.ds(0, 2)], st_recv.at[k])
        for b in (2 * k, 2 * k + 1):
            both = [stats[q, b] for q in range(8)]
            top = functools.reduce(jnp.maximum, [v[0:1] for v in both])
            tot = sum(v[1:2] * jnp.exp(v[0:1] - top) for v in both)
            lse[b] = top + jnp.log(tot)

    iota8 = lax.broadcasted_iota(jnp.int32, (8, tb), 0)
    group8 = lax.broadcasted_iota(jnp.int32, (groups, 8, tb), 0) * 8

    def backward(k, col, half):
        b = 2 * k + col
        acc = far if col else near
        phys = y + col * (1 - 2 * y)
        if half == 0:
            acc[k] = jnp.zeros((4, d, tc), F32)
        norm = jnp.broadcast_to(lse[place(k, col)], (8, tb))[None]
        ids = jnp.concatenate([t_all[2 * q + phys][:, k * tc:(k + 1) * tc] for q in range(4)], axis=1)
        rel = ids - vocab * (mate if half else r)
        rel = jnp.where((rel >= 0) & (rel < vocab), rel, -2 * vp)
        rel8 = jnp.broadcast_to(rel, (8, tb)) - iota8

        def tile_step(i, _):
            rows = pl.ds(pl.multiple_of(i * tile, tile), tile)
            zv = tile_logits(b, i)
            hit = (rel8 - (i - half * nt) * tile)[None] == group8
            zt_acc[...] += jnp.sum(jnp.where(hit, zv, 0.0), axis=0)
            dz = mask_pad(jnp.exp(zv - norm) - jnp.where(hit, 1.0, 0.0), i, 0.0)
            dz = dz.reshape(tile, tb).astype(BF16)
            part = jnp.dot(wt_all[i], dz, preferred_element_type=F32)
            for q in range(4):
                acc[k, q] += part[:, q * tc:(q + 1) * tc]
            dw[rows, :] += jnp.dot(dz, x_all[b].reshape(tb, d), preferred_element_type=F32)
            return 0

        lax.fori_loop(half * nt, (half + 1) * nt, tile_step, 0)
        if col == 1 and half == 1:
            for j in range(4):
                y_copy(k, dest(j)).start()

    def dest(j):
        return pick(z, [DESTS[q][j] for q in range(4)])

    def y_copy(k, zd):
        return remote(far.at[k, zd], far_in.at[k, zd], y_send.at[k, zd], y_recv.at[k, zd], across)

    def hop(k, j):
        zd = dest(j)
        drain(far_in.at[k, zd], y_recv.at[k, zd])

        def add_chain(slot):
            drain(chain.at[k, slot], c_recv.at[k, slot])
            near[k, zd] = near[k, zd] + far_in[k, zd] + chain[k, slot]

        def send(slot, dev):
            remote(near.at[k, zd], chain.at[k, slot], c_send.at[k, j], c_recv.at[k, slot], dev).start()

        if j < 3:
            passing = ((zd > z) & (z > 0)) | ((zd < z) & (z < 3))

            @pl.when(passing)
            def _():
                add_chain(zd)

            @pl.when(jnp.logical_not(passing))
            def _():
                near[k, zd] = near[k, zd] + far_in[k, zd]

            @pl.when(zd > z)
            def _():
                send(zd, right)

            @pl.when(zd == z - 1)
            def _():
                send(4, left)

            @pl.when(zd < z - 1)
            def _():
                send(zd, left)
        else:
            @pl.when((z > 0) & (z < 3))
            def _():
                drain(chain.at[k, z], c_recv.at[k, z])
                drain(chain.at[k, 4], c_recv.at[k, 4])
                near[k, z] = (near[k, z] + far_in[k, z]) + (chain[k, z] + chain[k, 4])

            @pl.when(z == 0)
            def _():
                add_chain(4)

            @pl.when(z == 3)
            def _():
                add_chain(3)

            out_copy(k).start()

    def out_copy(k):
        return pltpu.make_async_copy(near.at[k, z], dht_ref.at[k], out_sem.at[k])

    dw_copy = remote(dw.at[pl.ds(vp, vp)], dw_in, dw_sem.at[0], dw_sem.at[1], mate)
    dw_store = pltpu.make_async_copy(dw.at[pl.ds(0, vocab)], dw_out, out_sem.at[CHUNKS])

    def loss_copy(i):
        return remote(loss_rows.at[r], loss_rows.at[r], ls_send, ls_recv, (r + i) % 16)

    def send_grads():
        dw_copy.start()
        rows = sum(lse[b] for b in range(8)) * jnp.where(chip == 0, 1.0, 0.0)
        loss_rows[r] = rows - jnp.sum(zt_acc[...], axis=0, keepdims=True)
        for i in range(1, 16):
            loss_copy(i).start()

    def add_dw():
        dw_copy.wait_recv()

        def step(i, _):
            rows = pl.ds(pl.multiple_of(i * tile, tile), tile)
            dw[rows, :] += dw_in[rows, :]
            return 0

        lax.fori_loop(0, nt, step, 0)
        dw_store.start()
        drain(loss_rows.at[pl.ds(0, 15)], ls_recv)
        total = sum(loss_rows[q] for q in range(16))
        loss_ref[...] = jnp.sum(total, axis=1, keepdims=True) * jnp.ones((1, 128), F32)

    def start(copy):
        copy.start()

    first_backward = [e[1] for e in SCHEDULE].index("bwd")
    for n, (who, kind, *args) in enumerate(SCHEDULE):
        if n == first_backward:
            drain(t_all.at[pl.ds(0, 7)], t_recv)

        def run(kind=kind, args=args):
            if kind == "own":
                own(args[0], start)
            elif kind == "ag":
                gather(*args)
            elif kind == "hop":
                hop(*args)
            elif kind == "prep":
                prepare()
            elif kind == "fwd":
                forward(*args)
            elif kind == "stat":
                combine(*args)
            elif kind == "bwd":
                backward(*args)
            elif kind == "dw_send":
                send_grads()
            else:
                add_dw()

        if who == "A":
            run()
        else:
            pl.when(((z == 0) | (z == 3)) if who == "E" else ((z == 1) | (z == 2)))(run)

    def finish(copy):
        copy.wait_send()

    drain(loss_rows.at[pl.ds(0, 15)], ls_send)
    drain(stats.at[pl.ds(0, 7)], st_send)
    drain(t_all.at[pl.ds(0, 7)], t_send)
    for k in range(CHUNKS):
        own(k, finish)
        for j in range(7):
            relay(k, j, finish)
        for zd in range(4):
            y_copy(k, zd).wait_send()
        for j in range(3):
            drain(near.at[k, 0], c_send.at[k, j])
        out_copy(k).wait()
    dw_copy.wait_send()
    dw_store.wait()


def solution(mesh, tile=512):
    groups = mesh.shape["fsdp"]
    tok_spec = P(("dp", "fsdp"), None)

    def local_head(hidden, targets, weight):
        tb, d = hidden.shape
        tc = tb // CHUNKS
        vocab = weight.shape[0]
        vp = -(-vocab // tile) * tile
        nt = vp // tile
        dma = pltpu.SemaphoreType.DMA
        vmem = pltpu.VMEM
        loss, dht, dw = pl.pallas_call(
            functools.partial(head_kernel, vocab, tile),
            out_shape=(jax.ShapeDtypeStruct((1, 128), F32), jax.ShapeDtypeStruct((CHUNKS, d, tc), F32), jax.ShapeDtypeStruct((vocab, d), F32)),
            in_specs=[pl.BlockSpec(memory_space=vmem)] * 3,
            out_specs=(pl.BlockSpec(memory_space=vmem), pl.BlockSpec(memory_space=pl.ANY), pl.BlockSpec(memory_space=pl.ANY)),
            scratch_shapes=[
                vmem((8, 4, tc, d), BF16), vmem((8, d, tb), BF16), vmem((8, 1, tb), jnp.int32),
                vmem((2 * vp, d), BF16), vmem((2 * nt, d, tile), BF16),
                vmem((2 * vp, d), F32), vmem((vp, d), F32),
                vmem((CHUNKS, 4, d, tc), F32), vmem((CHUNKS, 4, d, tc), F32), vmem((CHUNKS, 4, d, tc), F32), vmem((CHUNKS, 5, d, tc), F32),
                vmem((8, 8, 2, tb), F32), vmem((8, 1, tb), F32), vmem((8, tb), F32), vmem((16, 1, tb), F32),
                dma((8, 4)), dma((3, CHUNKS, 8)), dma, dma, dma((2,)), dma((CHUNKS,)), dma, dma, dma,
                dma((CHUNKS, 4)), dma((CHUNKS, 4)), dma((CHUNKS, 3)), dma((CHUNKS, 5)), dma((2,)), dma((CHUNKS + 1,)),
            ],
            compiler_params=pltpu.CompilerParams(collective_id=0, has_side_effects=True, vmem_limit_bytes=66_000_000),
        )(hidden, targets.reshape(1, tb), weight)
        scale = 1.0 / (tb * groups)
        dh = dht.transpose(0, 2, 1).reshape(tb, d)
        return loss[0, :1] * scale, dh * scale, dw * scale

    return jax.shard_map(local_head, mesh=mesh, in_specs=(tok_spec, P(("dp", "fsdp")), P("fsdp", None)), out_specs=(P("dp"), tok_spec, tok_spec), check_vma=False)
```

```python
import functools

import jax
import jax.numpy as jnp
from jax import lax
from jax.experimental import pallas as pl
from jax.experimental.pallas import tpu as pltpu
from jax.sharding import PartitionSpec as P

MESH = pl.DeviceIdType.MESH
BF16, F32 = jnp.bfloat16, jnp.float32
CHUNKS = 4
COLUMN = ((1, 2, 3), (2, 0, 3), (1, 3, 0), (2, 1, 0))
DESTS = ((3, 2, 1, 0), (2, 3, 0, 1), (1, 0, 3, 2), (0, 1, 2, 3))
Y_FIRST = (0, 1, 1, 1)
SCHEDULE = (
    ('A', 'own', 0), ('A', 'prep', 2.5), ('I', 'own', 1), ('I', 'ag', 0, 1), ('E', 'own', 1), ('I', 'ag', 0, 0),
    ('I', 'ag', 0, 2), ('E', 'ag', 0, 0), ('E', 'ag', 0, 2), ('E', 'ag', 1, 0), ('I', 'own', 3), ('E', 'ag', 0, 3),
    ('E', 'own', 3), ('I', 'ag', 1, 3), ('E', 'ag', 1, 1), ('A', 'ag', 0, 4), ('I', 'ag', 1, 1), ('A', 'fwd', 0, 0),
    ('E', 'ag', 1, 3), ('I', 'ag', 1, 4), ('E', 'own', 2), ('I', 'ag', 1, 5), ('E', 'ag', 0, 1), ('E', 'ag', 0, 5),
    ('E', 'ag', 0, 6), ('I', 'ag', 0, 3), ('I', 'ag', 0, 5), ('I', 'ag', 3, 3), ('I', 'ag', 1, 0), ('E', 'ag', 3, 0),
    ('I', 'own', 2), ('I', 'ag', 0, 6), ('A', 'fwd', 0, 1), ('E', 'ag', 2, 0), ('I', 'ag', 1, 6), ('E', 'ag', 1, 5),
    ('E', 'ag', 3, 1), ('A', 'fwd', 1, 0), ('I', 'ag', 1, 2), ('A', 'stat', 0), ('I', 'ag', 3, 4), ('I', 'ag', 3, 5),
    ('A', 'bwd', 0, 1), ('E', 'ag', 1, 2), ('I', 'ag', 3, 1), ('E', 'ag', 1, 4), ('E', 'ag', 1, 6), ('I', 'ag', 2, 4),
    ('A', 'fwd', 1, 1), ('I', 'ag', 3, 0), ('I', 'ag', 2, 3), ('I', 'ag', 3, 6), ('A', 'bwd', 0, 0),
    ('I', 'ag', 2, 0), ('E', 'ag', 3, 3), ('I', 'ag', 2, 6), ('E', 'ag', 3, 2), ('A', 'stat', 1), ('E', 'hop', 0, 0),
    ('A', 'bwd', 1, 1), ('I', 'ag', 2, 2), ('I', 'ag', 3, 2), ('E', 'ag', 2, 6), ('E', 'hop', 0, 1),
    ('I', 'ag', 2, 5), ('E', 'ag', 3, 5), ('E', 'ag', 2, 1), ('I', 'hop', 0, 1), ('A', 'bwd', 1, 0),
    ('E', 'ag', 3, 4), ('E', 'ag', 2, 2), ('I', 'hop', 0, 0), ('I', 'ag', 2, 1), ('E', 'hop', 0, 2),
    ('E', 'hop', 1, 0), ('E', 'ag', 3, 6), ('E', 'ag', 2, 4), ('A', 'fwd', 3, 0), ('I', 'hop', 0, 2),
    ('A', 'fwd', 3, 1), ('E', 'ag', 2, 3), ('A', 'fwd', 2, 1), ('E', 'hop', 1, 1), ('A', 'stat', 3),
    ('A', 'bwd', 3, 1), ('E', 'hop', 1, 2), ('E', 'ag', 2, 5), ('I', 'hop', 0, 3), ('I', 'hop', 1, 0),
    ('A', 'fwd', 2, 0), ('A', 'bwd', 3, 0), ('E', 'hop', 3, 0), ('A', 'stat', 2), ('E', 'hop', 3, 1),
    ('I', 'hop', 1, 1), ('A', 'bwd', 2, 1), ('I', 'hop', 3, 1), ('E', 'hop', 3, 2), ('A', 'bwd', 2, 0),
    ('A', 'dw_send'), ('E', 'hop', 2, 0), ('I', 'hop', 3, 2), ('I', 'hop', 3, 0), ('E', 'hop', 2, 1),
    ('I', 'hop', 1, 3), ('E', 'hop', 2, 2), ('E', 'hop', 1, 3), ('E', 'hop', 0, 3), ('I', 'hop', 2, 1),
    ('I', 'hop', 1, 2), ('E', 'hop', 3, 3), ('E', 'hop', 2, 3), ('I', 'hop', 2, 0), ('I', 'hop', 2, 2),
    ('A', 'dw_add'), ('I', 'hop', 3, 3), ('I', 'hop', 2, 3),
)


def pick(z, table):
    lo, hi = z % 2, z // 2
    return table[0] * (1 - lo) * (1 - hi) + table[1] * lo * (1 - hi) + table[2] * (1 - lo) * hi + table[3] * lo * hi


def head_kernel(vocab, tile, h_ref, t_ref, w_ref, loss_ref, dht_ref, dw_out, x_all, xt_all, t_all, w_all, wt_all, dw, dw_in,
                far, near, far_in, chain, stats, lse, zt_acc, loss_rows, z_even, z_odd,
                x_recv, x_send, t_recv, t_send, w_sem, st_recv, st_send, ls_recv, ls_send, y_send, y_recv, c_send, c_recv,
                dw_sem, out_sem):
    tb, d = h_ref.shape
    tc = tb // CHUNKS
    vp = w_all.shape[0] // 2
    nt = vp // tile
    groups = tile // 8
    half_tile = tile // 2
    r = lax.axis_index("fsdp")
    c, chip = r % 2, r // 2
    y, z = chip % 2, chip // 2
    mate, across, left, right = r + 1 - 2 * c, r + 2 - 4 * y, r - 4, r + 4

    def remote(src, dst, ss, rs, dev):
        return pltpu.make_async_remote_copy(src_ref=src, dst_ref=dst, send_sem=ss, recv_sem=rs, device_id={"fsdp": dev}, device_id_type=MESH)

    def drain(ref, sem):
        pltpu.make_async_copy(ref, ref, sem).wait()

    barrier = pltpu.get_barrier_semaphore()
    for i in range(1, 16):
        pl.semaphore_signal(barrier, inc=1, device_id={"fsdp": (r + i) % 16}, device_id_type=MESH)

    for k in range(CHUNKS):
        x_all[2 * k, z] = h_ref[k * tc:(k + 1) * tc, :]
    t_all[chip] = t_ref[...]
    w_all[pl.ds(vp - tile, tile), :] = jnp.zeros((tile, d), BF16)
    w_all[pl.ds(0, vocab), :] = w_ref[...]

    def transpose_w(i, _):
        wt_all[i] = w_all[pl.ds(pl.multiple_of(i * tile, tile), tile), :].T
        return 0

    def zero_dw(i, _):
        dw[pl.ds(pl.multiple_of(i * tile, tile), tile), :] = jnp.zeros((tile, d), F32)
        return 0

    lax.fori_loop(0, nt, transpose_w, 0)
    pl.semaphore_wait(barrier, 15)

    w_copy = remote(w_all.at[pl.ds(0, vp)], w_all.at[pl.ds(vp, vp)], w_sem.at[0], w_sem.at[1], mate)

    def t_copy(i):
        return remote(t_all.at[chip], t_all.at[chip], t_send, t_recv, (2 * chip + 2 * i) % 16 + c)

    def prepare():
        for i in range(1, 8):
            t_copy(i).start()
        w_copy.start()
        lax.fori_loop(0, 2 * nt, zero_dw, 0)
        zt_acc[...] = jnp.zeros_like(zt_acc)
        w_copy.wait()
        lax.fori_loop(nt, 2 * nt, transpose_w, 0)

    def x_copy(k, col, zs, way, slot):
        dev = (across, left, right)[way]
        to = 1 if way == 0 else col
        return remote(x_all.at[2 * k + col, zs], x_all.at[2 * k + to, zs], x_send.at[way, k, slot], x_recv.at[2 * k + to, zs], dev)

    def along(k, col, zs, slot, to_left, to_right, act):
        @pl.when(to_left)
        def _():
            act(x_copy(k, col, zs, 1, slot))

        @pl.when(to_right)
        def _():
            act(x_copy(k, col, zs, 2, slot))

    def own(k, act):
        act(x_copy(k, 0, z, 0, 7))
        along(k, 0, z, 7, z > 0, z < 3, act)

    def arrival(k, j):
        if Y_FIRST[k]:
            col, n = (1, 0, 1, 0, 1, 0, 1)[j], (None, 0, 0, 1, 1, 2, 2)[j]
        else:
            col, n = (0, 1, 0, 1, 0, 1, 1)[j], (0, None, 1, 0, 2, 1, 2)[j]
        return col, z if n is None else pick(z, [COLUMN[q][n] for q in range(4)])

    def relay(k, j, act):
        col, zs = arrival(k, j)
        if Y_FIRST[k]:
            along(k, col, zs, j, (zs >= z) & (z > 0), (zs <= z) & (z < 3), act)
        elif col == 0:
            act(x_copy(k, 0, zs, 0, j))
            along(k, 0, zs, j, (zs > z) & (z > 0), (zs < z) & (z < 3), act)

    def gather(k, j):
        col, zs = arrival(k, j)
        drain(x_all.at[2 * k + col, zs], x_recv.at[2 * k + col, zs])
        relay(k, j, lambda copy: copy.start())

    def tile_logits(b, i):
        rows = pl.ds(pl.multiple_of(i * tile, tile), tile)
        return jnp.dot(w_all[rows, :], xt_all[b], preferred_element_type=F32).reshape(groups, 8, tb)

    def mask_pad(vals, i, fill, size):
        last = vp // size - 1
        live = (vocab - last * size) // 8
        if live == size // 8:
            return vals
        is_last = (jnp.zeros((size // 8 - live, 8, tb), jnp.int32) + i % (last + 1)) == last
        return jnp.concatenate([vals[:live], jnp.where(is_last, fill, vals[live:])], axis=0)

    def place(k, col):
        return 2 * k + y + col * (1 - 2 * y)

    def forward(k, col):
        b = 2 * k + col
        xt_all[b] = x_all[b].reshape(tb, d).T

        def logits_into(buf, i):
            rows = pl.ds(pl.multiple_of(i * half_tile, half_tile), half_tile)
            buf[...] = jnp.dot(w_all[rows, :], xt_all[b], preferred_element_type=F32)

        def update(buf, i, carry):
            m, s = carry
            zv = mask_pad(buf[...].reshape(half_tile // 8, 8, tb), i, -jnp.inf, half_tile)
            m_new = jnp.maximum(m, jnp.max(zv, axis=0))
            return m_new, s * jnp.exp(m - m_new) + jnp.sum(jnp.exp(zv - m_new[None]), axis=0)

        def pair(j, carry):
            logits_into(z_odd, 2 * j + 1)
            carry = update(z_even, 2 * j, carry)
            logits_into(z_even, 2 * j + 2)
            return update(z_odd, 2 * j + 1, carry)

        logits_into(z_even, 0)
        pairs = 2 * vp // (2 * half_tile)
        carry = (jnp.full((8, tb), -jnp.inf, F32), jnp.zeros((8, tb), F32))
        carry = lax.fori_loop(0, pairs - 1, pair, carry)
        logits_into(z_odd, 2 * pairs - 1)
        carry = update(z_even, 2 * pairs - 2, carry)
        m, s = update(z_odd, 2 * pairs - 1, carry)
        m1 = jnp.max(m, axis=0, keepdims=True)
        s1 = jnp.sum(s * jnp.exp(m - m1), axis=0, keepdims=True)
        p = place(k, col)
        stats[chip, p] = jnp.concatenate([m1, s1], axis=0)
        for i in range(1, 8):
            remote(stats.at[chip, p], stats.at[chip, p], st_send, st_recv.at[k], (2 * chip + 2 * i) % 16 + c).start()

    def combine(k):
        drain(stats.at[pl.ds(0, 7), pl.ds(0, 2)], st_recv.at[k])
        for b in (2 * k, 2 * k + 1):
            both = [stats[q, b] for q in range(8)]
            top = functools.reduce(jnp.maximum, [v[0:1] for v in both])
            tot = sum(v[1:2] * jnp.exp(v[0:1] - top) for v in both)
            lse[b] = top + jnp.log(tot)

    iota8 = lax.broadcasted_iota(jnp.int32, (8, tb), 0)
    group8 = lax.broadcasted_iota(jnp.int32, (groups, 8, tb), 0) * 8

    def backward(k, col):
        b = 2 * k + col
        acc = far if col else near
        phys = y + col * (1 - 2 * y)
        acc[k] = jnp.zeros((4, d, tc), F32)
        norm = jnp.broadcast_to(lse[place(k, col)], (8, tb))[None]
        ids = jnp.concatenate([t_all[2 * q + phys][:, k * tc:(k + 1) * tc] for q in range(4)], axis=1)

        def tile_step(i, _):
            slot = i // nt
            rel = ids - vocab * (r * (1 - slot) + mate * slot)
            rel = jnp.where((rel >= 0) & (rel < vocab), rel - (i % nt) * tile, -2 * vp)
            rows = pl.ds(pl.multiple_of(i * tile, tile), tile)
            zv = tile_logits(b, i)
            hit = (jnp.broadcast_to(rel, (8, tb)) - iota8)[None] == group8
            zt_acc[...] += jnp.sum(jnp.where(hit, zv, 0.0), axis=0)
            dz = mask_pad(jnp.exp(zv - norm) - jnp.where(hit, 1.0, 0.0), i, 0.0, tile)
            dz = dz.reshape(tile, tb).astype(BF16)
            part = jnp.dot(wt_all[i], dz, preferred_element_type=F32)
            for q in range(4):
                acc[k, q] += part[:, q * tc:(q + 1) * tc]
            dw[rows, :] += jnp.dot(dz, x_all[b].reshape(tb, d), preferred_element_type=F32)
            return 0

        lax.fori_loop(0, 2 * nt, tile_step, 0)
        if col:
            for j in range(4):
                y_copy(k, dest(j)).start()

    def dest(j):
        return pick(z, [DESTS[q][j] for q in range(4)])

    def y_copy(k, zd):
        return remote(far.at[k, zd], far_in.at[k, zd], y_send.at[k, zd], y_recv.at[k, zd], across)

    def hop(k, j):
        zd = dest(j)
        drain(far_in.at[k, zd], y_recv.at[k, zd])

        def add_chain(slot):
            drain(chain.at[k, slot], c_recv.at[k, slot])
            near[k, zd] = near[k, zd] + far_in[k, zd] + chain[k, slot]

        def send(slot, dev):
            remote(near.at[k, zd], chain.at[k, slot], c_send.at[k, j], c_recv.at[k, slot], dev).start()

        if j < 3:
            passing = ((zd > z) & (z > 0)) | ((zd < z) & (z < 3))

            @pl.when(passing)
            def _():
                add_chain(zd)

            @pl.when(jnp.logical_not(passing))
            def _():
                near[k, zd] = near[k, zd] + far_in[k, zd]

            @pl.when(zd > z)
            def _():
                send(zd, right)

            @pl.when(zd == z - 1)
            def _():
                send(4, left)

            @pl.when(zd < z - 1)
            def _():
                send(zd, left)
        else:
            @pl.when((z > 0) & (z < 3))
            def _():
                drain(chain.at[k, z], c_recv.at[k, z])
                drain(chain.at[k, 4], c_recv.at[k, 4])
                near[k, z] = (near[k, z] + far_in[k, z]) + (chain[k, z] + chain[k, 4])

            @pl.when(z == 0)
            def _():
                add_chain(4)

            @pl.when(z == 3)
            def _():
                add_chain(3)

            out_copy(k).start()

    def out_copy(k):
        return pltpu.make_async_copy(near.at[k, z], dht_ref.at[k], out_sem.at[k])

    dw_copy = remote(dw.at[pl.ds(vp, vp)], dw_in, dw_sem.at[0], dw_sem.at[1], mate)
    dw_store = pltpu.make_async_copy(dw.at[pl.ds(0, vocab)], dw_out, out_sem.at[CHUNKS])

    def loss_copy(i):
        return remote(loss_rows.at[r], loss_rows.at[r], ls_send, ls_recv, (r + i) % 16)

    def send_grads():
        dw_copy.start()
        rows = sum(lse[b] for b in range(8)) * jnp.where(chip == 0, 1.0, 0.0)
        loss_rows[r] = rows - jnp.sum(zt_acc[...], axis=0, keepdims=True)
        for i in range(1, 16):
            loss_copy(i).start()

    def add_dw():
        dw_copy.wait_recv()

        def step(i, _):
            rows = pl.ds(pl.multiple_of(i * tile, tile), tile)
            dw[rows, :] += dw_in[rows, :]
            return 0

        lax.fori_loop(0, nt, step, 0)
        dw_store.start()
        drain(loss_rows.at[pl.ds(0, 15)], ls_recv)
        total = sum(loss_rows[q] for q in range(16))
        loss_ref[...] = jnp.sum(total, axis=1, keepdims=True) * jnp.ones((1, 128), F32)

    def start(copy):
        copy.start()

    first_backward = [e[1] for e in SCHEDULE].index("bwd")
    for n, (who, kind, *args) in enumerate(SCHEDULE):
        if n == first_backward:
            drain(t_all.at[pl.ds(0, 7)], t_recv)

        def run(kind=kind, args=args):
            if kind == "own":
                own(args[0], start)
            elif kind == "ag":
                gather(*args)
            elif kind == "hop":
                hop(*args)
            elif kind == "prep":
                prepare()
            elif kind == "fwd":
                forward(*args)
            elif kind == "stat":
                combine(*args)
            elif kind == "bwd":
                backward(*args)
            elif kind == "dw_send":
                send_grads()
            else:
                add_dw()

        if who == "A":
            run()
        else:
            pl.when(((z == 0) | (z == 3)) if who == "E" else ((z == 1) | (z == 2)))(run)

    def finish(copy):
        copy.wait_send()

    drain(loss_rows.at[pl.ds(0, 15)], ls_send)
    drain(stats.at[pl.ds(0, 7)], st_send)
    drain(t_all.at[pl.ds(0, 7)], t_send)
    for k in range(CHUNKS):
        own(k, finish)
        for j in range(7):
            relay(k, j, finish)
        for zd in range(4):
            y_copy(k, zd).wait_send()
        for j in range(3):
            drain(near.at[k, 0], c_send.at[k, j])
        out_copy(k).wait()
    dw_copy.wait_send()
    dw_store.wait()


def solution(mesh, tile=1024):
    groups = mesh.shape["fsdp"]
    tok_spec = P(("dp", "fsdp"), None)

    def local_head(hidden, targets, weight):
        tb, d = hidden.shape
        tc = tb // CHUNKS
        vocab = weight.shape[0]
        vp = -(-vocab // tile) * tile
        nt = vp // tile
        dma = pltpu.SemaphoreType.DMA
        vmem = pltpu.VMEM
        loss, dht, dw = pl.pallas_call(
            functools.partial(head_kernel, vocab, tile),
            out_shape=(jax.ShapeDtypeStruct((1, 128), F32), jax.ShapeDtypeStruct((CHUNKS, d, tc), F32), jax.ShapeDtypeStruct((vocab, d), F32)),
            in_specs=[pl.BlockSpec(memory_space=vmem)] * 3,
            out_specs=(pl.BlockSpec(memory_space=vmem), pl.BlockSpec(memory_space=pl.ANY), pl.BlockSpec(memory_space=pl.ANY)),
            scratch_shapes=[
                vmem((8, 4, tc, d), BF16), vmem((8, d, tb), BF16), vmem((8, 1, tb), jnp.int32),
                vmem((2 * vp, d), BF16), vmem((2 * nt, d, tile), BF16),
                vmem((2 * vp, d), F32), vmem((vp, d), F32),
                vmem((CHUNKS, 4, d, tc), F32), vmem((CHUNKS, 4, d, tc), F32), vmem((CHUNKS, 4, d, tc), F32), vmem((CHUNKS, 5, d, tc), F32),
                vmem((8, 8, 2, tb), F32), vmem((8, 1, tb), F32), vmem((8, tb), F32), vmem((16, 1, tb), F32),
                vmem((tile // 2, tb), F32), vmem((tile // 2, tb), F32),
                dma((8, 4)), dma((3, CHUNKS, 8)), dma, dma, dma((2,)), dma((CHUNKS,)), dma, dma, dma,
                dma((CHUNKS, 4)), dma((CHUNKS, 4)), dma((CHUNKS, 3)), dma((CHUNKS, 5)), dma((2,)), dma((CHUNKS + 1,)),
            ],
            compiler_params=pltpu.CompilerParams(collective_id=0, has_side_effects=True, vmem_limit_bytes=66_000_000),
        )(hidden, targets.reshape(1, tb), weight)
        scale = 1.0 / (tb * groups)
        dh = dht.transpose(0, 2, 1).reshape(tb, d)
        return loss[0, :1] * scale, dh * scale, dw * scale

    return jax.shard_map(local_head, mesh=mesh, in_specs=(tok_spec, P(("dp", "fsdp")), P("fsdp", None)), out_specs=(P("dp"), tok_spec, tok_spec), check_vma=False)
```

```python
import functools

import jax
import jax.numpy as jnp
from jax import lax
from jax.experimental import pallas as pl
from jax.experimental.pallas import tpu as pltpu
from jax.sharding import PartitionSpec as P

MESH = pl.DeviceIdType.MESH
BF16, F32 = jnp.bfloat16, jnp.float32
CHUNKS = 4
COLUMN = ((1, 2, 3), (2, 0, 3), (1, 3, 0), (2, 1, 0))
DESTS = ((3, 2, 1, 0), (3, 0, 2, 1), (0, 3, 1, 2), (0, 1, 2, 3))
Y_FIRST = (0, 0, 1, 1)
SCHEDULE = (
    ('I', 'own', 0), ('I', 'own', 2), ('E', 'own', 0), ('I', 'ag', 0, 2), ('E', 'own', 1), ('E', 'own', 2),
    ('E', 'ag', 1, 1), ('E', 'ag', 2, 1), ('I', 'ag', 0, 0), ('E', 'own', 3), ('E', 'ag', 0, 0), ('A', 'prep', 2.5),
    ('I', 'own', 1), ('I', 'ag', 0, 4), ('E', 'ag', 2, 0), ('I', 'ag', 0, 1), ('E', 'ag', 0, 3), ('I', 'ag', 2, 3),
    ('E', 'ag', 0, 4), ('I', 'ag', 1, 2), ('E', 'ag', 0, 2), ('A', 'fwd', 0, 0), ('I', 'ag', 2, 1), ('E', 'ag', 3, 0),
    ('E', 'ag', 2, 3), ('E', 'ag', 1, 0), ('I', 'ag', 2, 5), ('I', 'ag', 0, 3), ('I', 'ag', 1, 4), ('I', 'ag', 1, 0),
    ('I', 'ag', 2, 4), ('I', 'ag', 0, 5), ('E', 'ag', 2, 5), ('A', 'fwd', 2, 0), ('E', 'ag', 0, 5), ('E', 'ag', 0, 1),
    ('I', 'ag', 2, 0), ('I', 'ag', 1, 1), ('I', 'ag', 1, 5), ('A', 'ag', 0, 6), ('E', 'ag', 1, 4), ('I', 'ag', 3, 4),
    ('A', 'fwd', 0, 1), ('I', 'ag', 2, 6), ('I', 'own', 3), ('E', 'ag', 1, 2), ('A', 'fwd', 1, 0), ('A', 'stat', 0),
    ('E', 'ag', 1, 6), ('E', 'ag', 1, 5), ('A', 'ag', 1, 3), ('I', 'ag', 2, 2), ('I', 'ag', 1, 6), ('A', 'fwd', 1, 1),
    ('A', 'bwd', 0, 1), ('I', 'ag', 3, 6), ('A', 'stat', 1), ('E', 'ag', 2, 4), ('I', 'ys', 0, 1), ('E', 'ag', 2, 6),
    ('E', 'ag', 2, 2), ('I', 'ag', 3, 1), ('I', 'ag', 3, 3), ('E', 'ys', 0, 1), ('A', 'fwd', 2, 1),
    ('A', 'bwd', 1, 1), ('I', 'ys', 0, 0), ('A', 'stat', 2), ('E', 'ys', 1, 0), ('E', 'ys', 1, 1), ('E', 'ys', 0, 2),
    ('I', 'ag', 3, 5), ('I', 'ys', 1, 1), ('I', 'ag', 3, 0), ('A', 'bwd', 2, 1), ('E', 'ys', 0, 0), ('I', 'ys', 2, 1),
    ('I', 'ys', 1, 0), ('E', 'ys', 2, 0), ('E', 'ag', 3, 2), ('E', 'ys', 0, 3), ('I', 'ys', 1, 2), ('I', 'ys', 2, 0),
    ('A', 'bwd', 1, 0), ('E', 'ag', 3, 5), ('I', 'ag', 3, 2), ('E', 'hop', 1, 1), ('E', 'hop', 1, 0),
    ('A', 'bwd', 0, 0), ('E', 'ag', 3, 4), ('E', 'ag', 3, 6), ('E', 'hop', 0, 1), ('A', 'fwd', 3, 1),
    ('E', 'ag', 3, 3), ('E', 'ys', 2, 1), ('E', 'ag', 3, 1), ('I', 'ys', 0, 2), ('A', 'fwd', 3, 0), ('I', 'ys', 2, 2),
    ('E', 'hop', 0, 0), ('I', 'hop', 1, 0), ('E', 'ys', 1, 2), ('E', 'ys', 2, 2), ('E', 'hop', 0, 2),
    ('A', 'bwd', 2, 0), ('I', 'hop', 0, 0), ('I', 'ys', 1, 3), ('A', 'stat', 3), ('E', 'hop', 2, 0),
    ('E', 'hop', 2, 1), ('I', 'hop', 1, 2), ('I', 'ys', 2, 3), ('E', 'ys', 1, 3), ('I', 'hop', 1, 1),
    ('A', 'bwd', 3, 1), ('A', 'ys', 3, 0), ('I', 'ys', 3, 2), ('I', 'ys', 3, 1), ('I', 'hop', 0, 2),
    ('I', 'ys', 0, 3), ('I', 'ys', 3, 3), ('I', 'hop', 2, 0), ('E', 'ys', 3, 1), ('I', 'hop', 0, 1),
    ('E', 'ys', 2, 3), ('I', 'hop', 2, 2), ('E', 'ys', 3, 2), ('E', 'hop', 2, 2), ('A', 'bwd', 3, 0),
    ('A', 'dw_send'), ('I', 'hop', 2, 1), ('A', 'hop', 3, 0), ('E', 'hop', 1, 3), ('E', 'hop', 3, 1),
    ('E', 'hop', 1, 2), ('I', 'hop', 3, 2), ('I', 'hop', 2, 3), ('I', 'hop', 3, 1), ('I', 'hop', 0, 3),
    ('E', 'hop', 2, 3), ('I', 'hop', 1, 3), ('E', 'hop', 0, 3), ('E', 'ys', 3, 3), ('E', 'hop', 3, 2),
    ('A', 'dw_add'), ('A', 'hop', 3, 3),
)


def pick(z, table):
    lo, hi = z % 2, z // 2
    return table[0] * (1 - lo) * (1 - hi) + table[1] * lo * (1 - hi) + table[2] * (1 - lo) * hi + table[3] * lo * hi


def head_kernel(vocab, tile, h_ref, t_ref, w_ref, loss_ref, dht_ref, dw_out, x_all, xt_all, t_all, w_all, wt_all, dw, dw_in,
                far, near, far_in, chain, stats, lse, zt_acc, loss_rows, z_even, z_odd,
                x_recv, x_send, t_recv, t_send, w_sem, st_recv, st_send, ls_recv, ls_send, y_send, y_recv, c_send, c_recv,
                dw_sem, out_sem):
    tb, d = h_ref.shape
    tc = tb // CHUNKS
    vp = w_all.shape[0] // 2
    nt = vp // tile
    groups = tile // 8
    half_tile = tile // 2
    r = lax.axis_index("fsdp")
    c, chip = r % 2, r // 2
    y, z = chip % 2, chip // 2
    mate, across, left, right = r + 1 - 2 * c, r + 2 - 4 * y, r - 4, r + 4

    def remote(src, dst, ss, rs, dev):
        return pltpu.make_async_remote_copy(src_ref=src, dst_ref=dst, send_sem=ss, recv_sem=rs, device_id={"fsdp": dev}, device_id_type=MESH)

    def drain(ref, sem):
        pltpu.make_async_copy(ref, ref, sem).wait()

    barrier = pltpu.get_barrier_semaphore()
    for i in range(1, 16):
        pl.semaphore_signal(barrier, inc=1, device_id={"fsdp": (r + i) % 16}, device_id_type=MESH)

    for k in range(CHUNKS):
        x_all[2 * k, z] = h_ref[k * tc:(k + 1) * tc, :]
    t_all[chip] = t_ref[...]
    w_all[pl.ds(vp - tile, tile), :] = jnp.zeros((tile, d), BF16)
    w_all[pl.ds(0, vocab), :] = w_ref[...]

    def transpose_w(i, _):
        wt_all[i] = w_all[pl.ds(pl.multiple_of(i * tile, tile), tile), :].T
        return 0

    def zero_dw(i, _):
        dw[pl.ds(pl.multiple_of(i * tile, tile), tile), :] = jnp.zeros((tile, d), F32)
        return 0

    lax.fori_loop(0, nt, transpose_w, 0)
    pl.semaphore_wait(barrier, 15)

    w_copy = remote(w_all.at[pl.ds(0, vp)], w_all.at[pl.ds(vp, vp)], w_sem.at[0], w_sem.at[1], mate)

    def t_copy(i):
        return remote(t_all.at[chip], t_all.at[chip], t_send, t_recv, (2 * chip + 2 * i) % 16 + c)

    def prepare():
        for i in range(1, 8):
            t_copy(i).start()
        w_copy.start()
        lax.fori_loop(0, 2 * nt, zero_dw, 0)
        zt_acc[...] = jnp.zeros_like(zt_acc)
        w_copy.wait()
        lax.fori_loop(nt, 2 * nt, transpose_w, 0)

    def x_copy(k, col, zs, way, slot):
        dev = (across, left, right)[way]
        to = 1 if way == 0 else col
        return remote(x_all.at[2 * k + col, zs], x_all.at[2 * k + to, zs], x_send.at[way, k, slot], x_recv.at[2 * k + to, zs], dev)

    def along(k, col, zs, slot, to_left, to_right, act):
        @pl.when(to_left)
        def _():
            act(x_copy(k, col, zs, 1, slot))

        @pl.when(to_right)
        def _():
            act(x_copy(k, col, zs, 2, slot))

    def own(k, act):
        act(x_copy(k, 0, z, 0, 7))
        along(k, 0, z, 7, z > 0, z < 3, act)

    def arrival(k, j):
        if Y_FIRST[k]:
            col, n = (1, 0, 1, 0, 1, 0, 1)[j], (None, 0, 0, 1, 1, 2, 2)[j]
        else:
            col, n = (0, 1, 0, 1, 0, 1, 1)[j], (0, None, 1, 0, 2, 1, 2)[j]
        return col, z if n is None else pick(z, [COLUMN[q][n] for q in range(4)])

    def relay(k, j, act):
        col, zs = arrival(k, j)
        if Y_FIRST[k]:
            along(k, col, zs, j, (zs >= z) & (z > 0), (zs <= z) & (z < 3), act)
        elif col == 0:
            act(x_copy(k, 0, zs, 0, j))
            along(k, 0, zs, j, (zs > z) & (z > 0), (zs < z) & (z < 3), act)

    def gather(k, j):
        col, zs = arrival(k, j)
        drain(x_all.at[2 * k + col, zs], x_recv.at[2 * k + col, zs])
        relay(k, j, lambda copy: copy.start())

    def tile_logits(b, i):
        rows = pl.ds(pl.multiple_of(i * tile, tile), tile)
        return jnp.dot(w_all[rows, :], xt_all[b], preferred_element_type=F32).reshape(groups, 8, tb)

    def mask_pad(vals, i, fill, size):
        last = vp // size - 1
        live = (vocab - last * size) // 8
        if live == size // 8:
            return vals
        is_last = (jnp.zeros((size // 8 - live, 8, tb), jnp.int32) + i % (last + 1)) == last
        return jnp.concatenate([vals[:live], jnp.where(is_last, fill, vals[live:])], axis=0)

    def place(k, col):
        return 2 * k + y + col * (1 - 2 * y)

    def forward(k, col):
        b = 2 * k + col
        xt_all[b] = x_all[b].reshape(tb, d).T

        def logits_into(buf, i):
            rows = pl.ds(pl.multiple_of(i * half_tile, half_tile), half_tile)
            buf[...] = jnp.dot(w_all[rows, :], xt_all[b], preferred_element_type=F32)

        def update(buf, i, carry):
            m, s = carry
            zv = mask_pad(buf[...].reshape(half_tile // 8, 8, tb), i, -jnp.inf, half_tile)
            m_new = jnp.maximum(m, jnp.max(zv, axis=0))
            return m_new, s * jnp.exp(m - m_new) + jnp.sum(jnp.exp(zv - m_new[None]), axis=0)

        def pair(j, carry):
            logits_into(z_odd, 2 * j + 1)
            carry = update(z_even, 2 * j, carry)
            logits_into(z_even, 2 * j + 2)
            return update(z_odd, 2 * j + 1, carry)

        logits_into(z_even, 0)
        pairs = 2 * vp // (2 * half_tile)
        carry = (jnp.full((8, tb), -jnp.inf, F32), jnp.zeros((8, tb), F32))
        carry = lax.fori_loop(0, pairs - 1, pair, carry)
        logits_into(z_odd, 2 * pairs - 1)
        carry = update(z_even, 2 * pairs - 2, carry)
        m, s = update(z_odd, 2 * pairs - 1, carry)
        m1 = jnp.max(m, axis=0, keepdims=True)
        s1 = jnp.sum(s * jnp.exp(m - m1), axis=0, keepdims=True)
        p = place(k, col)
        stats[chip, p] = jnp.concatenate([m1, s1], axis=0)
        for i in range(1, 8):
            remote(stats.at[chip, p], stats.at[chip, p], st_send, st_recv.at[k], (2 * chip + 2 * i) % 16 + c).start()

    def combine(k):
        drain(stats.at[pl.ds(0, 7), pl.ds(0, 2)], st_recv.at[k])
        for b in (2 * k, 2 * k + 1):
            both = [stats[q, b] for q in range(8)]
            top = functools.reduce(jnp.maximum, [v[0:1] for v in both])
            tot = sum(v[1:2] * jnp.exp(v[0:1] - top) for v in both)
            lse[b] = top + jnp.log(tot)

    iota8 = lax.broadcasted_iota(jnp.int32, (8, tb), 0)
    group8 = lax.broadcasted_iota(jnp.int32, (groups, 8, tb), 0) * 8

    def backward(k, col):
        b = 2 * k + col
        acc = far if col else near
        phys = y + col * (1 - 2 * y)
        acc[k] = jnp.zeros((4, d, tc), F32)
        norm = jnp.broadcast_to(lse[place(k, col)], (8, tb))[None]
        ids = jnp.concatenate([t_all[2 * q + phys][:, k * tc:(k + 1) * tc] for q in range(4)], axis=1)

        def tile_step(i, _):
            slot = i // nt
            rel = ids - vocab * (r * (1 - slot) + mate * slot)
            rel = jnp.where((rel >= 0) & (rel < vocab), rel - (i % nt) * tile, -2 * vp)
            rows = pl.ds(pl.multiple_of(i * tile, tile), tile)
            zv = tile_logits(b, i)
            hit = (jnp.broadcast_to(rel, (8, tb)) - iota8)[None] == group8
            zt_acc[...] += jnp.sum(jnp.where(hit, zv, 0.0), axis=0)
            dz = mask_pad(jnp.exp(zv - norm) - jnp.where(hit, 1.0, 0.0), i, 0.0, tile)
            dz = dz.reshape(tile, tb).astype(BF16)
            part = jnp.dot(wt_all[i], dz, preferred_element_type=F32)
            for q in range(4):
                acc[k, q] += part[:, q * tc:(q + 1) * tc]
            dw[rows, :] += jnp.dot(dz, x_all[b].reshape(tb, d), preferred_element_type=F32)
            return 0

        lax.fori_loop(0, 2 * nt, tile_step, 0)

    def dest(j):
        return pick(z, [DESTS[q][j] for q in range(4)])

    def y_copy(k, zd):
        return remote(far.at[k, zd], far_in.at[k, zd], y_send.at[k, zd], y_recv.at[k, zd], across)

    def hop(k, j):
        zd = dest(j)
        drain(far_in.at[k, zd], y_recv.at[k, zd])

        def add_chain(slot):
            drain(chain.at[k, slot], c_recv.at[k, slot])
            near[k, zd] = near[k, zd] + far_in[k, zd] + chain[k, slot]

        def send(slot, dev):
            remote(near.at[k, zd], chain.at[k, slot], c_send.at[k, j], c_recv.at[k, slot], dev).start()

        if j < 3:
            passing = ((zd > z) & (z > 0)) | ((zd < z) & (z < 3))

            @pl.when(passing)
            def _():
                add_chain(zd)

            @pl.when(jnp.logical_not(passing))
            def _():
                near[k, zd] = near[k, zd] + far_in[k, zd]

            @pl.when(zd > z)
            def _():
                send(zd, right)

            @pl.when(zd == z - 1)
            def _():
                send(4, left)

            @pl.when(zd < z - 1)
            def _():
                send(zd, left)
        else:
            @pl.when((z > 0) & (z < 3))
            def _():
                drain(chain.at[k, z], c_recv.at[k, z])
                drain(chain.at[k, 4], c_recv.at[k, 4])
                near[k, z] = (near[k, z] + far_in[k, z]) + (chain[k, z] + chain[k, 4])

            @pl.when(z == 0)
            def _():
                add_chain(4)

            @pl.when(z == 3)
            def _():
                add_chain(3)

            out_copy(k).start()

    def out_copy(k):
        return pltpu.make_async_copy(near.at[k, z], dht_ref.at[k], out_sem.at[k])

    dw_copy = remote(dw.at[pl.ds(vp, vp)], dw_in, dw_sem.at[0], dw_sem.at[1], mate)
    dw_store = pltpu.make_async_copy(dw.at[pl.ds(0, vocab)], dw_out, out_sem.at[CHUNKS])

    def loss_copy(i):
        return remote(loss_rows.at[r], loss_rows.at[r], ls_send, ls_recv, (r + i) % 16)

    def send_grads():
        dw_copy.start()
        rows = sum(lse[b] for b in range(8)) * jnp.where(chip == 0, 1.0, 0.0)
        loss_rows[r] = rows - jnp.sum(zt_acc[...], axis=0, keepdims=True)
        for i in range(1, 16):
            loss_copy(i).start()

    def add_dw():
        dw_copy.wait_recv()

        def step(i, _):
            rows = pl.ds(pl.multiple_of(i * tile, tile), tile)
            dw[rows, :] += dw_in[rows, :]
            return 0

        lax.fori_loop(0, nt, step, 0)
        dw_store.start()
        drain(loss_rows.at[pl.ds(0, 15)], ls_recv)
        total = sum(loss_rows[q] for q in range(16))
        loss_ref[...] = jnp.sum(total, axis=1, keepdims=True) * jnp.ones((1, 128), F32)

    def start(copy):
        copy.start()

    first_backward = [e[1] for e in SCHEDULE].index("bwd")
    for n, (who, kind, *args) in enumerate(SCHEDULE):
        if n == first_backward:
            drain(t_all.at[pl.ds(0, 7)], t_recv)

        def run(kind=kind, args=args):
            if kind == "own":
                own(args[0], start)
            elif kind == "ag":
                gather(*args)
            elif kind == "hop":
                hop(*args)
            elif kind == "ys":
                y_copy(args[0], dest(args[1])).start()
            elif kind == "prep":
                prepare()
            elif kind == "fwd":
                forward(*args)
            elif kind == "stat":
                combine(*args)
            elif kind == "bwd":
                backward(*args)
            elif kind == "dw_send":
                send_grads()
            else:
                add_dw()

        if who == "A":
            run()
        else:
            pl.when(((z == 0) | (z == 3)) if who == "E" else ((z == 1) | (z == 2)))(run)

    def finish(copy):
        copy.wait_send()

    drain(loss_rows.at[pl.ds(0, 15)], ls_send)
    drain(stats.at[pl.ds(0, 7)], st_send)
    drain(t_all.at[pl.ds(0, 7)], t_send)
    for k in range(CHUNKS):
        own(k, finish)
        for j in range(7):
            relay(k, j, finish)
        for zd in range(4):
            y_copy(k, zd).wait_send()
        for j in range(3):
            drain(near.at[k, 0], c_send.at[k, j])
        out_copy(k).wait()
    dw_copy.wait_send()
    dw_store.wait()


def solution(mesh, tile=1024):
    groups = mesh.shape["fsdp"]
    tok_spec = P(("dp", "fsdp"), None)

    def local_head(hidden, targets, weight):
        tb, d = hidden.shape
        tc = tb // CHUNKS
        vocab = weight.shape[0]
        vp = -(-vocab // tile) * tile
        nt = vp // tile
        dma = pltpu.SemaphoreType.DMA
        vmem = pltpu.VMEM
        loss, dht, dw = pl.pallas_call(
            functools.partial(head_kernel, vocab, tile),
            out_shape=(jax.ShapeDtypeStruct((1, 128), F32), jax.ShapeDtypeStruct((CHUNKS, d, tc), F32), jax.ShapeDtypeStruct((vocab, d), F32)),
            in_specs=[pl.BlockSpec(memory_space=vmem)] * 3,
            out_specs=(pl.BlockSpec(memory_space=vmem), pl.BlockSpec(memory_space=pl.ANY), pl.BlockSpec(memory_space=pl.ANY)),
            scratch_shapes=[
                vmem((8, 4, tc, d), BF16), vmem((8, d, tb), BF16), vmem((8, 1, tb), jnp.int32),
                vmem((2 * vp, d), BF16), vmem((2 * nt, d, tile), BF16),
                vmem((2 * vp, d), F32), vmem((vp, d), F32),
                vmem((CHUNKS, 4, d, tc), F32), vmem((CHUNKS, 4, d, tc), F32), vmem((CHUNKS, 4, d, tc), F32), vmem((CHUNKS, 5, d, tc), F32),
                vmem((8, 8, 2, tb), F32), vmem((8, 1, tb), F32), vmem((8, tb), F32), vmem((16, 1, tb), F32),
                vmem((tile // 2, tb), F32), vmem((tile // 2, tb), F32),
                dma((8, 4)), dma((3, CHUNKS, 8)), dma, dma, dma((2,)), dma((CHUNKS,)), dma, dma, dma,
                dma((CHUNKS, 4)), dma((CHUNKS, 4)), dma((CHUNKS, 3)), dma((CHUNKS, 5)), dma((2,)), dma((CHUNKS + 1,)),
            ],
            compiler_params=pltpu.CompilerParams(collective_id=0, has_side_effects=True, vmem_limit_bytes=66_000_000),
        )(hidden, targets.reshape(1, tb), weight)
        scale = 1.0 / (tb * groups)
        dh = dht.transpose(0, 2, 1).reshape(tb, d)
        return loss[0, :1] * scale, dh * scale, dw * scale

    return jax.shard_map(local_head, mesh=mesh, in_specs=(tok_spec, P(("dp", "fsdp")), P("fsdp", None)), out_specs=(P("dp"), tok_spec, tok_spec), check_vma=False)
```

```python
import functools

import jax
import jax.numpy as jnp
from jax import lax
from jax.experimental import pallas as pl
from jax.experimental.pallas import tpu as pltpu
from jax.sharding import PartitionSpec as P

MESH = pl.DeviceIdType.MESH
BF16, F32 = jnp.bfloat16, jnp.float32
CHUNKS = 4
COLUMN = ((1, 2, 3), (2, 0, 3), (1, 3, 0), (2, 1, 0))
DESTS = ((3, 2, 1, 0), (3, 2, 0, 1), (0, 1, 3, 2), (0, 1, 2, 3))
Y_FIRST = (0, 1, 1, 1)
SCHEDULE = (
    ('A', 'own', 0), ('A', 'prep', 2.5), ('E', 'own', 1), ('E', 'own', 2), ('E', 'ag', 0, 0), ('I', 'own', 1),
    ('E', 'ag', 1, 0), ('E', 'ag', 2, 0), ('A', 'ag', 0, 2), ('E', 'ag', 0, 3), ('E', 'ag', 1, 2), ('E', 'ag', 0, 4),
    ('I', 'ag', 0, 1), ('I', 'ag', 0, 0), ('I', 'ag', 1, 3), ('I', 'ag', 1, 0), ('E', 'own', 3), ('E', 'ag', 0, 1),
    ('I', 'ag', 0, 4), ('I', 'ag', 0, 5), ('A', 'fwd', 0, 0), ('I', 'ag', 2, 3), ('I', 'ag', 1, 1), ('I', 'ag', 1, 4),
    ('I', 'ag', 0, 6), ('I', 'ag', 0, 3), ('E', 'ag', 0, 5), ('I', 'ag', 1, 5), ('E', 'ag', 1, 1), ('E', 'ag', 0, 6),
    ('I', 'ag', 2, 4), ('A', 'fwd', 0, 1), ('E', 'ag', 1, 5), ('I', 'ag', 1, 2), ('I', 'ag', 1, 6), ('I', 'own', 2),
    ('I', 'own', 3), ('E', 'ag', 1, 3), ('A', 'fwd', 1, 0), ('E', 'ag', 1, 4), ('E', 'ag', 1, 6), ('I', 'ag', 2, 0),
    ('A', 'fwd', 1, 1), ('A', 'stat', 0), ('I', 'ag', 2, 1), ('A', 'bwd', 0, 1), ('E', 'ys', 0, 0), ('I', 'ys', 0, 1),
    ('I', 'ag', 3, 0), ('I', 'ag', 2, 2), ('I', 'ag', 2, 5), ('A', 'stat', 1), ('E', 'ys', 0, 2), ('E', 'ag', 2, 3),
    ('I', 'ag', 3, 3), ('A', 'bwd', 0, 0), ('I', 'ys', 0, 2), ('I', 'ys', 0, 0), ('E', 'ag', 2, 1), ('I', 'ag', 2, 6),
    ('E', 'ag', 2, 2), ('E', 'ag', 3, 0), ('E', 'hop', 0, 0), ('E', 'ag', 2, 5), ('E', 'ys', 0, 1),
    ('A', 'bwd', 1, 1), ('E', 'ag', 2, 6), ('E', 'hop', 0, 2), ('A', 'ys', 1, 1), ('I', 'ag', 3, 5),
    ('A', 'fwd', 2, 0), ('E', 'ag', 2, 4), ('E', 'hop', 0, 1), ('I', 'ag', 3, 4), ('A', 'fwd', 2, 1),
    ('E', 'ag', 3, 5), ('E', 'ys', 1, 0), ('I', 'ag', 3, 1), ('I', 'ys', 1, 0), ('A', 'bwd', 1, 0), ('E', 'ag', 3, 2),
    ('I', 'ys', 1, 3), ('E', 'hop', 1, 0), ('E', 'ys', 1, 3), ('I', 'ag', 3, 6), ('I', 'ag', 3, 2),
    ('I', 'hop', 0, 0), ('A', 'stat', 2), ('E', 'ys', 1, 2), ('I', 'ys', 0, 3), ('E', 'ag', 3, 3), ('A', 'bwd', 2, 1),
    ('E', 'ys', 2, 0), ('E', 'ag', 3, 1), ('E', 'ag', 3, 6), ('E', 'hop', 1, 1), ('I', 'ys', 1, 2),
    ('I', 'hop', 0, 1), ('E', 'ag', 3, 4), ('A', 'fwd', 3, 1), ('I', 'ys', 2, 0), ('A', 'fwd', 3, 0),
    ('I', 'hop', 0, 2), ('A', 'ys', 2, 1), ('I', 'hop', 1, 0), ('A', 'ys', 2, 2), ('E', 'hop', 1, 2),
    ('A', 'bwd', 2, 0), ('E', 'hop', 2, 1), ('I', 'hop', 0, 3), ('E', 'hop', 2, 0), ('A', 'stat', 3),
    ('I', 'hop', 1, 2), ('I', 'hop', 1, 1), ('E', 'ys', 0, 3), ('A', 'bwd', 3, 1), ('I', 'ys', 3, 0),
    ('I', 'hop', 2, 1), ('I', 'hop', 2, 0), ('I', 'ys', 3, 2), ('E', 'hop', 2, 2), ('I', 'ys', 3, 1),
    ('E', 'ys', 3, 0), ('E', 'ys', 3, 1), ('E', 'ys', 3, 2), ('A', 'bwd', 3, 0), ('A', 'dw_send'), ('E', 'hop', 3, 0),
    ('I', 'hop', 2, 2), ('I', 'hop', 3, 0), ('I', 'ys', 2, 3), ('E', 'hop', 0, 3), ('E', 'hop', 3, 1),
    ('I', 'ys', 3, 3), ('A', 'hop', 1, 3), ('I', 'hop', 3, 1), ('I', 'hop', 3, 2), ('I', 'hop', 2, 3),
    ('E', 'ys', 3, 3), ('E', 'hop', 3, 2), ('E', 'ys', 2, 3), ('E', 'hop', 2, 3), ('A', 'dw_add'), ('A', 'hop', 3, 3),
)


def pick(z, table):
    lo, hi = z % 2, z // 2
    return table[0] * (1 - lo) * (1 - hi) + table[1] * lo * (1 - hi) + table[2] * (1 - lo) * hi + table[3] * lo * hi


def head_kernel(vocab, tile, h_ref, t_ref, w_ref, loss_ref, dht_ref, dw_out, x_all, xt_all, t_all, w_all, wt_all, dw, dw_in,
                far, near, far_in, chain, stats, lse, zt_acc, loss_rows, z_even, z_odd,
                x_recv, x_send, t_recv, t_send, w_sem, st_recv, st_send, ls_recv, ls_send, y_send, y_recv, c_send, c_recv,
                dw_sem, out_sem):
    tb, d = h_ref.shape
    tc = tb // CHUNKS
    vp = w_all.shape[0] // 2
    nt = vp // tile
    groups = tile // 8
    half_tile = tile // 2
    r = lax.axis_index("fsdp")
    c, chip = r % 2, r // 2
    y, z = chip % 2, chip // 2
    mate, across, left, right = r + 1 - 2 * c, r + 2 - 4 * y, r - 4, r + 4

    def remote(src, dst, ss, rs, dev):
        return pltpu.make_async_remote_copy(src_ref=src, dst_ref=dst, send_sem=ss, recv_sem=rs, device_id={"fsdp": dev}, device_id_type=MESH)

    def drain(ref, sem):
        pltpu.make_async_copy(ref, ref, sem).wait()

    barrier = pltpu.get_barrier_semaphore()
    for i in range(1, 16):
        pl.semaphore_signal(barrier, inc=1, device_id={"fsdp": (r + i) % 16}, device_id_type=MESH)

    for k in range(CHUNKS):
        x_all[2 * k, z] = h_ref[k * tc:(k + 1) * tc, :]
    t_all[chip] = t_ref[...]
    w_all[pl.ds(vp - tile, tile), :] = jnp.zeros((tile, d), BF16)
    w_all[pl.ds(0, vocab), :] = w_ref[...]

    def transpose_w(i, _):
        wt_all[i] = w_all[pl.ds(pl.multiple_of(i * tile, tile), tile), :].T
        return 0

    def zero_dw(i, _):
        dw[pl.ds(pl.multiple_of(i * tile, tile), tile), :] = jnp.zeros((tile, d), F32)
        return 0

    lax.fori_loop(0, nt, transpose_w, 0)
    pl.semaphore_wait(barrier, 15)

    w_copy = remote(w_all.at[pl.ds(0, vp)], w_all.at[pl.ds(vp, vp)], w_sem.at[0], w_sem.at[1], mate)

    def t_copy(i):
        return remote(t_all.at[chip], t_all.at[chip], t_send, t_recv, (2 * chip + 2 * i) % 16 + c)

    def prepare():
        for i in range(1, 8):
            t_copy(i).start()
        w_copy.start()
        lax.fori_loop(0, 2 * nt, zero_dw, 0)
        zt_acc[...] = jnp.zeros_like(zt_acc)
        w_copy.wait()
        lax.fori_loop(nt, 2 * nt, transpose_w, 0)

    def x_copy(k, col, zs, way, slot):
        dev = (across, left, right)[way]
        to = 1 if way == 0 else col
        return remote(x_all.at[2 * k + col, zs], x_all.at[2 * k + to, zs], x_send.at[way, k, slot], x_recv.at[2 * k + to, zs], dev)

    def along(k, col, zs, slot, to_left, to_right, act):
        @pl.when(to_left)
        def _():
            act(x_copy(k, col, zs, 1, slot))

        @pl.when(to_right)
        def _():
            act(x_copy(k, col, zs, 2, slot))

    def own(k, act):
        act(x_copy(k, 0, z, 0, 7))
        along(k, 0, z, 7, z > 0, z < 3, act)

    def arrival(k, j):
        if Y_FIRST[k]:
            col, n = (1, 0, 1, 0, 1, 0, 1)[j], (None, 0, 0, 1, 1, 2, 2)[j]
        else:
            col, n = (0, 1, 0, 1, 0, 1, 1)[j], (0, None, 1, 0, 2, 1, 2)[j]
        return col, z if n is None else pick(z, [COLUMN[q][n] for q in range(4)])

    def relay(k, j, act):
        col, zs = arrival(k, j)
        if Y_FIRST[k]:
            along(k, col, zs, j, (zs >= z) & (z > 0), (zs <= z) & (z < 3), act)
        elif col == 0:
            act(x_copy(k, 0, zs, 0, j))
            along(k, 0, zs, j, (zs > z) & (z > 0), (zs < z) & (z < 3), act)

    def gather(k, j):
        col, zs = arrival(k, j)
        drain(x_all.at[2 * k + col, zs], x_recv.at[2 * k + col, zs])
        relay(k, j, lambda copy: copy.start())

    def tile_logits(b, i):
        rows = pl.ds(pl.multiple_of(i * tile, tile), tile)
        return jnp.dot(w_all[rows, :], xt_all[b], preferred_element_type=F32).reshape(groups, 8, tb)

    def mask_pad(vals, i, fill, size):
        last = vp // size - 1
        live = (vocab - last * size) // 8
        if live == size // 8:
            return vals
        is_last = (jnp.zeros((size // 8 - live, 8, tb), jnp.int32) + i % (last + 1)) == last
        return jnp.concatenate([vals[:live], jnp.where(is_last, fill, vals[live:])], axis=0)

    def place(k, col):
        return 2 * k + y + col * (1 - 2 * y)

    def forward(k, col):
        b = 2 * k + col
        xt_all[b] = x_all[b].reshape(tb, d).T

        def logits_into(buf, i):
            rows = pl.ds(pl.multiple_of(i * half_tile, half_tile), half_tile)
            buf[...] = jnp.dot(w_all[rows, :], xt_all[b], preferred_element_type=F32)

        def update(buf, i, carry):
            m, s = carry
            zv = mask_pad(buf[...].reshape(half_tile // 8, 8, tb), i, -jnp.inf, half_tile)
            m_new = jnp.maximum(m, jnp.max(zv, axis=0))
            return m_new, s * jnp.exp(m - m_new) + jnp.sum(jnp.exp(zv - m_new[None]), axis=0)

        def pair(j, carry):
            logits_into(z_odd, 2 * j + 1)
            carry = update(z_even, 2 * j, carry)
            logits_into(z_even, 2 * j + 2)
            return update(z_odd, 2 * j + 1, carry)

        logits_into(z_even, 0)
        pairs = 2 * vp // (2 * half_tile)
        carry = (jnp.full((8, tb), -jnp.inf, F32), jnp.zeros((8, tb), F32))
        carry = lax.fori_loop(0, pairs - 1, pair, carry)
        logits_into(z_odd, 2 * pairs - 1)
        carry = update(z_even, 2 * pairs - 2, carry)
        m, s = update(z_odd, 2 * pairs - 1, carry)
        m1 = jnp.max(m, axis=0, keepdims=True)
        s1 = jnp.sum(s * jnp.exp(m - m1), axis=0, keepdims=True)
        p = place(k, col)
        stats[chip, p] = jnp.concatenate([m1, s1], axis=0)
        for i in range(1, 8):
            remote(stats.at[chip, p], stats.at[chip, p], st_send, st_recv.at[k], (2 * chip + 2 * i) % 16 + c).start()

    def combine(k):
        drain(stats.at[pl.ds(0, 7), pl.ds(0, 2)], st_recv.at[k])
        for b in (2 * k, 2 * k + 1):
            both = [stats[q, b] for q in range(8)]
            top = functools.reduce(jnp.maximum, [v[0:1] for v in both])
            tot = sum(v[1:2] * jnp.exp(v[0:1] - top) for v in both)
            lse[b] = top + jnp.log(tot)

    iota8 = lax.broadcasted_iota(jnp.int32, (8, tb), 0)
    group8 = lax.broadcasted_iota(jnp.int32, (groups, 8, tb), 0) * 8

    def backward(k, col):
        b = 2 * k + col
        acc = far if col else near
        phys = y + col * (1 - 2 * y)
        acc[k] = jnp.zeros((4, d, tc), F32)
        norm = jnp.broadcast_to(lse[place(k, col)], (8, tb))[None]
        ids = jnp.concatenate([t_all[2 * q + phys][:, k * tc:(k + 1) * tc] for q in range(4)], axis=1)

        def tile_step(i, _):
            slot = i // nt
            rel = ids - vocab * (r * (1 - slot) + mate * slot)
            rel = jnp.where((rel >= 0) & (rel < vocab), rel - (i % nt) * tile, -2 * vp)
            rows = pl.ds(pl.multiple_of(i * tile, tile), tile)
            zv = tile_logits(b, i)
            hit = (jnp.broadcast_to(rel, (8, tb)) - iota8)[None] == group8
            zt_acc[...] += jnp.sum(jnp.where(hit, zv, 0.0), axis=0)
            dz = mask_pad(jnp.exp(zv - norm) - jnp.where(hit, 1.0, 0.0), i, 0.0, tile)
            dz = dz.reshape(tile, tb).astype(BF16)
            part = jnp.dot(wt_all[i], dz, preferred_element_type=F32)
            for q in range(4):
                acc[k, q] += part[:, q * tc:(q + 1) * tc]
            dw[rows, :] += jnp.dot(dz, x_all[b].reshape(tb, d), preferred_element_type=F32)
            return 0

        lax.fori_loop(0, 2 * nt, tile_step, 0)

    def dest(j):
        return pick(z, [DESTS[q][j] for q in range(4)])

    def y_copy(k, zd):
        return remote(far.at[k, zd], far_in.at[k, zd], y_send.at[k, zd], y_recv.at[k, zd], across)

    def hop(k, j):
        zd = dest(j)
        drain(far_in.at[k, zd], y_recv.at[k, zd])

        def add_chain(slot):
            drain(chain.at[k, slot], c_recv.at[k, slot])
            near[k, zd] = near[k, zd] + far_in[k, zd] + chain[k, slot]

        def send(slot, dev):
            remote(near.at[k, zd], chain.at[k, slot], c_send.at[k, j], c_recv.at[k, slot], dev).start()

        if j < 3:
            passing = ((zd > z) & (z > 0)) | ((zd < z) & (z < 3))

            @pl.when(passing)
            def _():
                add_chain(zd)

            @pl.when(jnp.logical_not(passing))
            def _():
                near[k, zd] = near[k, zd] + far_in[k, zd]

            @pl.when(zd > z)
            def _():
                send(zd, right)

            @pl.when(zd == z - 1)
            def _():
                send(4, left)

            @pl.when(zd < z - 1)
            def _():
                send(zd, left)
        else:
            @pl.when((z > 0) & (z < 3))
            def _():
                drain(chain.at[k, z], c_recv.at[k, z])
                drain(chain.at[k, 4], c_recv.at[k, 4])
                near[k, z] = (near[k, z] + far_in[k, z]) + (chain[k, z] + chain[k, 4])

            @pl.when(z == 0)
            def _():
                add_chain(4)

            @pl.when(z == 3)
            def _():
                add_chain(3)

            out_copy(k).start()

    def out_copy(k):
        return pltpu.make_async_copy(near.at[k, z], dht_ref.at[k], out_sem.at[k])

    dw_copy = remote(dw.at[pl.ds(vp, vp)], dw_in, dw_sem.at[0], dw_sem.at[1], mate)
    dw_store = pltpu.make_async_copy(dw.at[pl.ds(0, vocab)], dw_out, out_sem.at[CHUNKS])

    def loss_copy(i):
        return remote(loss_rows.at[r], loss_rows.at[r], ls_send, ls_recv, (r + i) % 16)

    def send_grads():
        dw_copy.start()
        rows = sum(lse[b] for b in range(8)) * jnp.where(chip == 0, 1.0, 0.0)
        loss_rows[r] = rows - jnp.sum(zt_acc[...], axis=0, keepdims=True)
        for i in range(1, 16):
            loss_copy(i).start()

    def add_dw():
        dw_copy.wait_recv()

        def step(i, _):
            rows = pl.ds(pl.multiple_of(i * tile, tile), tile)
            dw[rows, :] += dw_in[rows, :]
            return 0

        lax.fori_loop(0, nt, step, 0)
        dw_store.start()
        drain(loss_rows.at[pl.ds(0, 15)], ls_recv)
        total = sum(loss_rows[q] for q in range(16))
        loss_ref[...] = jnp.sum(total, axis=1, keepdims=True) * jnp.ones((1, 128), F32)

    def start(copy):
        copy.start()

    first_backward = [e[1] for e in SCHEDULE].index("bwd")
    for n, (who, kind, *args) in enumerate(SCHEDULE):
        if n == first_backward:
            drain(t_all.at[pl.ds(0, 7)], t_recv)

        def run(kind=kind, args=args):
            if kind == "own":
                own(args[0], start)
            elif kind == "ag":
                gather(*args)
            elif kind == "hop":
                hop(*args)
            elif kind == "ys":
                y_copy(args[0], dest(args[1])).start()
            elif kind == "prep":
                prepare()
            elif kind == "fwd":
                forward(*args)
            elif kind == "stat":
                combine(*args)
            elif kind == "bwd":
                backward(*args)
            elif kind == "dw_send":
                send_grads()
            else:
                add_dw()

        if who == "A":
            run()
        else:
            pl.when(((z == 0) | (z == 3)) if who == "E" else ((z == 1) | (z == 2)))(run)

    def finish(copy):
        copy.wait_send()

    drain(loss_rows.at[pl.ds(0, 15)], ls_send)
    drain(stats.at[pl.ds(0, 7)], st_send)
    drain(t_all.at[pl.ds(0, 7)], t_send)
    for k in range(CHUNKS):
        own(k, finish)
        for j in range(7):
            relay(k, j, finish)
        for zd in range(4):
            y_copy(k, zd).wait_send()
        for j in range(3):
            drain(near.at[k, 0], c_send.at[k, j])
        out_copy(k).wait()
    dw_copy.wait_send()
    dw_store.wait()


def finish_kernel(scale, dht_ref, dw_ref, dh_out, dw_out, dht, dh, dw, in_sem, out_sem):
    chunks, d, tc = dht.shape
    vocab = dw.shape[0]
    step = -(-vocab // 64) * 8
    spans = [pl.ds(lo, min(step, vocab - lo)) for lo in range(0, vocab, step)]
    loads = [pltpu.make_async_copy(dw_ref.at[s], dw.at[s], in_sem.at[n]) for n, s in enumerate(spans)]
    loads += [pltpu.make_async_copy(dht_ref.at[k], dht.at[k], in_sem.at[8 + k]) for k in range(chunks)]
    for load in loads:
        load.start()
    stores = []
    for n, s in enumerate(spans):
        loads[n].wait()
        dw[s, :] = dw[s, :] * scale
        stores.append(pltpu.make_async_copy(dw.at[s], dw_out.at[s], out_sem.at[n]))
        stores[-1].start()
    for k in range(chunks):
        loads[len(spans) + k].wait()
        rows = pl.ds(k * tc, tc)
        dh[rows, :] = dht[k].T * scale
        stores.append(pltpu.make_async_copy(dh.at[rows], dh_out.at[rows], out_sem.at[8 + k]))
        stores[-1].start()
    for store in stores:
        store.wait()


def solution(mesh, tile=1024):
    groups = mesh.shape["fsdp"]
    tok_spec = P(("dp", "fsdp"), None)

    def local_head(hidden, targets, weight):
        tb, d = hidden.shape
        tc = tb // CHUNKS
        vocab = weight.shape[0]
        vp = -(-vocab // tile) * tile
        nt = vp // tile
        dma = pltpu.SemaphoreType.DMA
        vmem = pltpu.VMEM
        loss, dht, dw = pl.pallas_call(
            functools.partial(head_kernel, vocab, tile),
            out_shape=(jax.ShapeDtypeStruct((1, 128), F32), jax.ShapeDtypeStruct((CHUNKS, d, tc), F32), jax.ShapeDtypeStruct((vocab, d), F32)),
            in_specs=[pl.BlockSpec(memory_space=vmem)] * 3,
            out_specs=(pl.BlockSpec(memory_space=vmem), pl.BlockSpec(memory_space=pl.ANY), pl.BlockSpec(memory_space=pl.ANY)),
            scratch_shapes=[
                vmem((8, 4, tc, d), BF16), vmem((8, d, tb), BF16), vmem((8, 1, tb), jnp.int32),
                vmem((2 * vp, d), BF16), vmem((2 * nt, d, tile), BF16),
                vmem((2 * vp, d), F32), vmem((vp, d), F32),
                vmem((CHUNKS, 4, d, tc), F32), vmem((CHUNKS, 4, d, tc), F32), vmem((CHUNKS, 4, d, tc), F32), vmem((CHUNKS, 5, d, tc), F32),
                vmem((8, 8, 2, tb), F32), vmem((8, 1, tb), F32), vmem((8, tb), F32), vmem((16, 1, tb), F32),
                vmem((tile // 2, tb), F32), vmem((tile // 2, tb), F32),
                dma((8, 4)), dma((3, CHUNKS, 8)), dma, dma, dma((2,)), dma((CHUNKS,)), dma, dma, dma,
                dma((CHUNKS, 4)), dma((CHUNKS, 4)), dma((CHUNKS, 3)), dma((CHUNKS, 5)), dma((2,)), dma((CHUNKS + 1,)),
            ],
            compiler_params=pltpu.CompilerParams(collective_id=0, has_side_effects=True, vmem_limit_bytes=66_000_000),
        )(hidden, targets.reshape(1, tb), weight)
        scale = 1.0 / (tb * groups)
        dh, dw = pl.pallas_call(
            functools.partial(finish_kernel, scale),
            out_shape=(jax.ShapeDtypeStruct((tb, d), F32), jax.ShapeDtypeStruct((vocab, d), F32)),
            in_specs=[pl.BlockSpec(memory_space=pl.ANY)] * 2,
            out_specs=(pl.BlockSpec(memory_space=pl.ANY), pl.BlockSpec(memory_space=pl.ANY)),
            scratch_shapes=[vmem((CHUNKS, d, tc), F32), vmem((tb, d), F32), vmem((vocab, d), F32), dma((8 + CHUNKS,)), dma((8 + CHUNKS,))],
        )(dht, dw)
        return loss[0, :1] * scale, dh, dw

    return jax.shard_map(local_head, mesh=mesh, in_specs=(tok_spec, P(("dp", "fsdp")), P("fsdp", None)), out_specs=(P("dp"), tok_spec, tok_spec), check_vma=False)
```

```python
import functools

import jax
import jax.numpy as jnp
from jax import lax
from jax.experimental import pallas as pl
from jax.experimental.pallas import tpu as pltpu
from jax.sharding import PartitionSpec as P

MESH = pl.DeviceIdType.MESH
BF16, F32 = jnp.bfloat16, jnp.float32
CHUNKS = 4
COLUMN = ((1, 2, 3), (2, 0, 3), (1, 3, 0), (2, 1, 0))
DESTS = ((3, 2, 1, 0), (3, 2, 0, 1), (0, 1, 3, 2), (0, 1, 2, 3))
Y_FIRST = (0, 1, 1, 1)
SCHEDULE = (
    ('A', 'own', 0), ('A', 'prep', 2.5), ('E', 'own', 1), ('E', 'own', 2), ('E', 'ag', 0, 0), ('I', 'own', 1),
    ('E', 'ag', 1, 0), ('E', 'ag', 2, 0), ('A', 'ag', 0, 2), ('E', 'ag', 0, 3), ('E', 'ag', 1, 2), ('E', 'ag', 0, 4),
    ('I', 'ag', 0, 1), ('I', 'ag', 0, 0), ('I', 'ag', 1, 3), ('I', 'ag', 1, 0), ('E', 'own', 3), ('E', 'ag', 0, 1),
    ('I', 'ag', 0, 4), ('I', 'ag', 0, 5), ('A', 'fwd', 0, 0), ('I', 'ag', 2, 3), ('I', 'ag', 1, 1), ('I', 'ag', 1, 4),
    ('I', 'ag', 0, 6), ('I', 'ag', 0, 3), ('E', 'ag', 0, 5), ('I', 'ag', 1, 5), ('E', 'ag', 1, 1), ('E', 'ag', 0, 6),
    ('I', 'ag', 2, 4), ('A', 'fwd', 0, 1), ('E', 'ag', 1, 5), ('I', 'ag', 1, 2), ('I', 'ag', 1, 6), ('I', 'own', 2),
    ('I', 'own', 3), ('E', 'ag', 1, 3), ('A', 'fwd', 1, 0), ('E', 'ag', 1, 4), ('E', 'ag', 1, 6), ('I', 'ag', 2, 0),
    ('A', 'fwd', 1, 1), ('A', 'stat', 0), ('I', 'ag', 2, 1), ('A', 'bwd', 0, 1), ('E', 'ys', 0, 0), ('I', 'ys', 0, 1),
    ('I', 'ag', 3, 0), ('I', 'ag', 2, 2), ('I', 'ag', 2, 5), ('A', 'stat', 1), ('E', 'ys', 0, 2), ('E', 'ag', 2, 3),
    ('I', 'ag', 3, 3), ('A', 'bwd', 0, 0), ('I', 'ys', 0, 2), ('I', 'ys', 0, 0), ('E', 'ag', 2, 1), ('I', 'ag', 2, 6),
    ('E', 'ag', 2, 2), ('E', 'ag', 3, 0), ('E', 'hop', 0, 0), ('E', 'ag', 2, 5), ('E', 'ys', 0, 1),
    ('A', 'bwd', 1, 1), ('E', 'ag', 2, 6), ('E', 'hop', 0, 2), ('A', 'ys', 1, 1), ('I', 'ag', 3, 5),
    ('A', 'fwd', 2, 0), ('E', 'ag', 2, 4), ('E', 'hop', 0, 1), ('I', 'ag', 3, 4), ('A', 'fwd', 2, 1),
    ('E', 'ag', 3, 5), ('E', 'ys', 1, 0), ('I', 'ag', 3, 1), ('I', 'ys', 1, 0), ('A', 'bwd', 1, 0), ('E', 'ag', 3, 2),
    ('I', 'ys', 1, 3), ('E', 'hop', 1, 0), ('E', 'ys', 1, 3), ('I', 'ag', 3, 6), ('I', 'ag', 3, 2),
    ('I', 'hop', 0, 0), ('A', 'stat', 2), ('E', 'ys', 1, 2), ('I', 'ys', 0, 3), ('E', 'ag', 3, 3), ('A', 'bwd', 2, 1),
    ('E', 'ys', 2, 0), ('E', 'ag', 3, 1), ('E', 'ag', 3, 6), ('E', 'hop', 1, 1), ('I', 'ys', 1, 2),
    ('I', 'hop', 0, 1), ('E', 'ag', 3, 4), ('A', 'fwd', 3, 1), ('I', 'ys', 2, 0), ('A', 'fwd', 3, 0),
    ('I', 'hop', 0, 2), ('A', 'ys', 2, 1), ('I', 'hop', 1, 0), ('A', 'ys', 2, 2), ('E', 'hop', 1, 2),
    ('A', 'bwd', 2, 0), ('E', 'hop', 2, 1), ('I', 'hop', 0, 3), ('E', 'hop', 2, 0), ('A', 'stat', 3),
    ('I', 'hop', 1, 2), ('I', 'hop', 1, 1), ('E', 'ys', 0, 3), ('A', 'bwd', 3, 1), ('I', 'ys', 3, 0),
    ('I', 'hop', 2, 1), ('I', 'hop', 2, 0), ('I', 'ys', 3, 2), ('E', 'hop', 2, 2), ('I', 'ys', 3, 1),
    ('E', 'ys', 3, 0), ('E', 'ys', 3, 1), ('E', 'ys', 3, 2), ('A', 'bwd', 3, 0), ('A', 'dw_send'), ('E', 'hop', 3, 0),
    ('I', 'hop', 2, 2), ('I', 'hop', 3, 0), ('I', 'ys', 2, 3), ('E', 'hop', 0, 3), ('E', 'hop', 3, 1),
    ('I', 'ys', 3, 3), ('A', 'hop', 1, 3), ('I', 'hop', 3, 1), ('I', 'hop', 3, 2), ('I', 'hop', 2, 3),
    ('E', 'ys', 3, 3), ('E', 'hop', 3, 2), ('E', 'ys', 2, 3), ('E', 'hop', 2, 3), ('A', 'dw_add'), ('A', 'hop', 3, 3),
)


def pick(z, table):
    lo, hi = z % 2, z // 2
    return table[0] * (1 - lo) * (1 - hi) + table[1] * lo * (1 - hi) + table[2] * (1 - lo) * hi + table[3] * lo * hi


def head_kernel(vocab, tile, h_ref, t_ref, w_ref, loss_ref, dht_ref, dw_out, x_all, xt_all, t_all, w_all, wt_all, dw, dw_in,
                far, near, far_in, chain, stats, lse, zt_acc, loss_rows, z_even, z_odd,
                x_recv, x_send, t_recv, t_send, w_sem, st_recv, st_send, ls_recv, ls_send, y_send, y_recv, c_send, c_recv,
                dw_sem, out_sem):
    tb, d = h_ref.shape
    tc = tb // CHUNKS
    vp = w_all.shape[0] // 2
    nt = vp // tile
    groups = tile // 8
    half_tile = tile // 2
    r = lax.axis_index("fsdp")
    c, chip = r % 2, r // 2
    y, z = chip % 2, chip // 2
    mate, across, left, right = r + 1 - 2 * c, r + 2 - 4 * y, r - 4, r + 4

    def remote(src, dst, ss, rs, dev):
        return pltpu.make_async_remote_copy(src_ref=src, dst_ref=dst, send_sem=ss, recv_sem=rs, device_id={"fsdp": dev}, device_id_type=MESH)

    def drain(ref, sem):
        pltpu.make_async_copy(ref, ref, sem).wait()

    barrier = pltpu.get_barrier_semaphore()
    for i in range(1, 16):
        pl.semaphore_signal(barrier, inc=1, device_id={"fsdp": (r + i) % 16}, device_id_type=MESH)

    for k in range(CHUNKS):
        x_all[2 * k, z] = h_ref[k * tc:(k + 1) * tc, :]
    t_all[chip] = t_ref[...]
    w_all[pl.ds(vp - tile, tile), :] = jnp.zeros((tile, d), BF16)
    w_all[pl.ds(0, vocab), :] = w_ref[...]

    def transpose_w(i, _):
        wt_all[i] = w_all[pl.ds(pl.multiple_of(i * tile, tile), tile), :].T
        return 0

    def zero_dw(i, _):
        dw[pl.ds(pl.multiple_of(i * tile, tile), tile), :] = jnp.zeros((tile, d), F32)
        return 0

    pl.semaphore_wait(barrier, 15)

    w_copy = remote(w_all.at[pl.ds(0, vp)], w_all.at[pl.ds(vp, vp)], w_sem.at[0], w_sem.at[1], mate)

    def t_copy(i):
        return remote(t_all.at[chip], t_all.at[chip], t_send, t_recv, (2 * chip + 2 * i) % 16 + c)

    def prepare():
        for i in range(1, 8):
            t_copy(i).start()
        w_copy.start()
        lax.fori_loop(0, 2 * nt, zero_dw, 0)
        zt_acc[...] = jnp.zeros_like(zt_acc)
        lax.fori_loop(0, nt, transpose_w, 0)

    def x_copy(k, col, zs, way, slot):
        dev = (across, left, right)[way]
        to = 1 if way == 0 else col
        return remote(x_all.at[2 * k + col, zs], x_all.at[2 * k + to, zs], x_send.at[way, k, slot], x_recv.at[2 * k + to, zs], dev)

    def along(k, col, zs, slot, to_left, to_right, act):
        @pl.when(to_left)
        def _():
            act(x_copy(k, col, zs, 1, slot))

        @pl.when(to_right)
        def _():
            act(x_copy(k, col, zs, 2, slot))

    def own(k, act):
        act(x_copy(k, 0, z, 0, 7))
        along(k, 0, z, 7, z > 0, z < 3, act)

    def arrival(k, j):
        if Y_FIRST[k]:
            col, n = (1, 0, 1, 0, 1, 0, 1)[j], (None, 0, 0, 1, 1, 2, 2)[j]
        else:
            col, n = (0, 1, 0, 1, 0, 1, 1)[j], (0, None, 1, 0, 2, 1, 2)[j]
        return col, z if n is None else pick(z, [COLUMN[q][n] for q in range(4)])

    def relay(k, j, act):
        col, zs = arrival(k, j)
        if Y_FIRST[k]:
            along(k, col, zs, j, (zs >= z) & (z > 0), (zs <= z) & (z < 3), act)
        elif col == 0:
            act(x_copy(k, 0, zs, 0, j))
            along(k, 0, zs, j, (zs > z) & (z > 0), (zs < z) & (z < 3), act)

    def gather(k, j):
        col, zs = arrival(k, j)
        drain(x_all.at[2 * k + col, zs], x_recv.at[2 * k + col, zs])
        relay(k, j, lambda copy: copy.start())

    def tile_logits(b, i):
        rows = pl.ds(pl.multiple_of(i * tile, tile), tile)
        return jnp.dot(w_all[rows, :], xt_all[b], preferred_element_type=F32).reshape(groups, 8, tb)

    def mask_pad(vals, i, fill, size):
        last = vp // size - 1
        live = (vocab - last * size) // 8
        if live == size // 8:
            return vals
        is_last = (jnp.zeros((size // 8 - live, 8, tb), jnp.int32) + i % (last + 1)) == last
        return jnp.concatenate([vals[:live], jnp.where(is_last, fill, vals[live:])], axis=0)

    def place(k, col):
        return 2 * k + y + col * (1 - 2 * y)

    def forward(k, col):
        b = 2 * k + col
        xt_all[b] = x_all[b].reshape(tb, d).T

        def logits_into(buf, i):
            rows = pl.ds(pl.multiple_of(i * half_tile, half_tile), half_tile)
            buf[...] = jnp.dot(w_all[rows, :], xt_all[b], preferred_element_type=F32)

        def update(buf, i, carry):
            m, s = carry
            zv = mask_pad(buf[...].reshape(half_tile // 8, 8, tb), i, -jnp.inf, half_tile)
            m_new = jnp.maximum(m, jnp.max(zv, axis=0))
            return m_new, s * jnp.exp(m - m_new) + jnp.sum(jnp.exp(zv - m_new[None]), axis=0)

        def pair(j, carry):
            logits_into(z_odd, 2 * j + 1)
            carry = update(z_even, 2 * j, carry)
            logits_into(z_even, 2 * j + 2)
            return update(z_odd, 2 * j + 1, carry)

        logits_into(z_even, 0)
        pairs = 2 * vp // (2 * half_tile)
        carry = (jnp.full((8, tb), -jnp.inf, F32), jnp.zeros((8, tb), F32))
        carry = lax.fori_loop(0, pairs - 1, pair, carry)
        logits_into(z_odd, 2 * pairs - 1)
        carry = update(z_even, 2 * pairs - 2, carry)
        m, s = update(z_odd, 2 * pairs - 1, carry)
        m1 = jnp.max(m, axis=0, keepdims=True)
        s1 = jnp.sum(s * jnp.exp(m - m1), axis=0, keepdims=True)
        p = place(k, col)
        stats[chip, p] = jnp.concatenate([m1, s1], axis=0)
        for i in range(1, 8):
            remote(stats.at[chip, p], stats.at[chip, p], st_send, st_recv.at[k], (2 * chip + 2 * i) % 16 + c).start()

    def combine(k):
        drain(stats.at[pl.ds(0, 7), pl.ds(0, 2)], st_recv.at[k])
        for b in (2 * k, 2 * k + 1):
            both = [stats[q, b] for q in range(8)]
            top = functools.reduce(jnp.maximum, [v[0:1] for v in both])
            tot = sum(v[1:2] * jnp.exp(v[0:1] - top) for v in both)
            lse[b] = top + jnp.log(tot)

    iota8 = lax.broadcasted_iota(jnp.int32, (8, tb), 0)
    group8 = lax.broadcasted_iota(jnp.int32, (groups, 8, tb), 0) * 8

    def backward(k, col):
        b = 2 * k + col
        acc = far if col else near
        phys = y + col * (1 - 2 * y)
        acc[k] = jnp.zeros((4, d, tc), F32)
        norm = jnp.broadcast_to(lse[place(k, col)], (8, tb))[None]
        ids = jnp.concatenate([t_all[2 * q + phys][:, k * tc:(k + 1) * tc] for q in range(4)], axis=1)

        def tile_step(i, _):
            slot = i // nt
            rel = ids - vocab * (r * (1 - slot) + mate * slot)
            rel = jnp.where((rel >= 0) & (rel < vocab), rel - (i % nt) * tile, -2 * vp)
            rows = pl.ds(pl.multiple_of(i * tile, tile), tile)
            zv = tile_logits(b, i)
            hit = (jnp.broadcast_to(rel, (8, tb)) - iota8)[None] == group8
            zt_acc[...] += jnp.sum(jnp.where(hit, zv, 0.0), axis=0)
            dz = mask_pad(jnp.exp(zv - norm) - jnp.where(hit, 1.0, 0.0), i, 0.0, tile)
            dz = dz.reshape(tile, tb).astype(BF16)
            part = jnp.dot(wt_all[i], dz, preferred_element_type=F32)
            for q in range(4):
                acc[k, q] += part[:, q * tc:(q + 1) * tc]
            dw[rows, :] += jnp.dot(dz, x_all[b].reshape(tb, d), preferred_element_type=F32)
            return 0

        lax.fori_loop(0, 2 * nt, tile_step, 0)

    def dest(j):
        return pick(z, [DESTS[q][j] for q in range(4)])

    def y_copy(k, zd):
        return remote(far.at[k, zd], far_in.at[k, zd], y_send.at[k, zd], y_recv.at[k, zd], across)

    def hop(k, j):
        zd = dest(j)
        drain(far_in.at[k, zd], y_recv.at[k, zd])

        def add_chain(slot):
            drain(chain.at[k, slot], c_recv.at[k, slot])
            near[k, zd] = near[k, zd] + far_in[k, zd] + chain[k, slot]

        def send(slot, dev):
            remote(near.at[k, zd], chain.at[k, slot], c_send.at[k, j], c_recv.at[k, slot], dev).start()

        if j < 3:
            passing = ((zd > z) & (z > 0)) | ((zd < z) & (z < 3))

            @pl.when(passing)
            def _():
                add_chain(zd)

            @pl.when(jnp.logical_not(passing))
            def _():
                near[k, zd] = near[k, zd] + far_in[k, zd]

            @pl.when(zd > z)
            def _():
                send(zd, right)

            @pl.when(zd == z - 1)
            def _():
                send(4, left)

            @pl.when(zd < z - 1)
            def _():
                send(zd, left)
        else:
            @pl.when((z > 0) & (z < 3))
            def _():
                drain(chain.at[k, z], c_recv.at[k, z])
                drain(chain.at[k, 4], c_recv.at[k, 4])
                near[k, z] = (near[k, z] + far_in[k, z]) + (chain[k, z] + chain[k, 4])

            @pl.when(z == 0)
            def _():
                add_chain(4)

            @pl.when(z == 3)
            def _():
                add_chain(3)

            out_copy(k).start()

    def out_copy(k):
        return pltpu.make_async_copy(near.at[k, z], dht_ref.at[k], out_sem.at[k])

    dw_copy = remote(dw.at[pl.ds(vp, vp)], dw_in, dw_sem.at[0], dw_sem.at[1], mate)
    dw_store = pltpu.make_async_copy(dw.at[pl.ds(0, vocab)], dw_out, out_sem.at[CHUNKS])

    def loss_copy(i):
        return remote(loss_rows.at[r], loss_rows.at[r], ls_send, ls_recv, (r + i) % 16)

    def send_grads():
        dw_copy.start()
        rows = sum(lse[b] for b in range(8)) * jnp.where(chip == 0, 1.0, 0.0)
        loss_rows[r] = rows - jnp.sum(zt_acc[...], axis=0, keepdims=True)
        for i in range(1, 16):
            loss_copy(i).start()

    def add_dw():
        dw_copy.wait_recv()

        def step(i, _):
            rows = pl.ds(pl.multiple_of(i * tile, tile), tile)
            dw[rows, :] += dw_in[rows, :]
            return 0

        lax.fori_loop(0, nt, step, 0)
        dw_store.start()
        drain(loss_rows.at[pl.ds(0, 15)], ls_recv)
        total = sum(loss_rows[q] for q in range(16))
        loss_ref[...] = jnp.sum(total, axis=1, keepdims=True) * jnp.ones((1, 128), F32)

    def start(copy):
        copy.start()

    kinds = [e[1] for e in SCHEDULE]
    first_forward, first_stat, first_backward = kinds.index("fwd"), kinds.index("stat"), kinds.index("bwd")
    for n, (who, kind, *args) in enumerate(SCHEDULE):
        if n == first_forward:
            w_copy.wait()
        if n == first_stat:
            lax.fori_loop(nt, 2 * nt, transpose_w, 0)
        if n == first_backward:
            drain(t_all.at[pl.ds(0, 7)], t_recv)

        def run(kind=kind, args=args):
            if kind == "own":
                own(args[0], start)
            elif kind == "ag":
                gather(*args)
            elif kind == "hop":
                hop(*args)
            elif kind == "ys":
                y_copy(args[0], dest(args[1])).start()
            elif kind == "prep":
                prepare()
            elif kind == "fwd":
                forward(*args)
            elif kind == "stat":
                combine(*args)
            elif kind == "bwd":
                backward(*args)
            elif kind == "dw_send":
                send_grads()
            else:
                add_dw()

        if who == "A":
            run()
        else:
            pl.when(((z == 0) | (z == 3)) if who == "E" else ((z == 1) | (z == 2)))(run)

    def finish(copy):
        copy.wait_send()

    drain(loss_rows.at[pl.ds(0, 15)], ls_send)
    drain(stats.at[pl.ds(0, 7)], st_send)
    drain(t_all.at[pl.ds(0, 7)], t_send)
    for k in range(CHUNKS):
        own(k, finish)
        for j in range(7):
            relay(k, j, finish)
        for zd in range(4):
            y_copy(k, zd).wait_send()
        for j in range(3):
            drain(near.at[k, 0], c_send.at[k, j])
        out_copy(k).wait()
    dw_copy.wait_send()
    dw_store.wait()


def finish_kernel(scale, dht_ref, dw_ref, dh_out, dw_out, dht, dh, dw, in_sem, out_sem):
    chunks, d, tc = dht.shape
    vocab = dw.shape[0]
    step = -(-vocab // 64) * 8
    spans = [pl.ds(lo, min(step, vocab - lo)) for lo in range(0, vocab, step)]
    loads = [pltpu.make_async_copy(dw_ref.at[s], dw.at[s], in_sem.at[n]) for n, s in enumerate(spans)]
    loads += [pltpu.make_async_copy(dht_ref.at[k], dht.at[k], in_sem.at[8 + k]) for k in range(chunks)]
    for load in loads:
        load.start()
    stores = []
    for n, s in enumerate(spans):
        loads[n].wait()
        dw[s, :] = dw[s, :] * scale
        stores.append(pltpu.make_async_copy(dw.at[s], dw_out.at[s], out_sem.at[n]))
        stores[-1].start()
    for k in range(chunks):
        loads[len(spans) + k].wait()
        rows = pl.ds(k * tc, tc)
        dh[rows, :] = dht[k].T * scale
        stores.append(pltpu.make_async_copy(dh.at[rows], dh_out.at[rows], out_sem.at[8 + k]))
        stores[-1].start()
    for store in stores:
        store.wait()


def solution(mesh, tile=1024):
    groups = mesh.shape["fsdp"]
    tok_spec = P(("dp", "fsdp"), None)

    def local_head(hidden, targets, weight):
        tb, d = hidden.shape
        tc = tb // CHUNKS
        vocab = weight.shape[0]
        vp = -(-vocab // tile) * tile
        nt = vp // tile
        dma = pltpu.SemaphoreType.DMA
        vmem = pltpu.VMEM
        loss, dht, dw = pl.pallas_call(
            functools.partial(head_kernel, vocab, tile),
            out_shape=(jax.ShapeDtypeStruct((1, 128), F32), jax.ShapeDtypeStruct((CHUNKS, d, tc), F32), jax.ShapeDtypeStruct((vocab, d), F32)),
            in_specs=[pl.BlockSpec(memory_space=vmem)] * 3,
            out_specs=(pl.BlockSpec(memory_space=vmem), pl.BlockSpec(memory_space=pl.ANY), pl.BlockSpec(memory_space=pl.ANY)),
            scratch_shapes=[
                vmem((8, 4, tc, d), BF16), vmem((8, d, tb), BF16), vmem((8, 1, tb), jnp.int32),
                vmem((2 * vp, d), BF16), vmem((2 * nt, d, tile), BF16),
                vmem((2 * vp, d), F32), vmem((vp, d), F32),
                vmem((CHUNKS, 4, d, tc), F32), vmem((CHUNKS, 4, d, tc), F32), vmem((CHUNKS, 4, d, tc), F32), vmem((CHUNKS, 5, d, tc), F32),
                vmem((8, 8, 2, tb), F32), vmem((8, 1, tb), F32), vmem((8, tb), F32), vmem((16, 1, tb), F32),
                vmem((tile // 2, tb), F32), vmem((tile // 2, tb), F32),
                dma((8, 4)), dma((3, CHUNKS, 8)), dma, dma, dma((2,)), dma((CHUNKS,)), dma, dma, dma,
                dma((CHUNKS, 4)), dma((CHUNKS, 4)), dma((CHUNKS, 3)), dma((CHUNKS, 5)), dma((2,)), dma((CHUNKS + 1,)),
            ],
            compiler_params=pltpu.CompilerParams(collective_id=0, has_side_effects=True, vmem_limit_bytes=66_000_000),
        )(hidden, targets.reshape(1, tb), weight)
        scale = 1.0 / (tb * groups)
        dh, dw = pl.pallas_call(
            functools.partial(finish_kernel, scale),
            out_shape=(jax.ShapeDtypeStruct((tb, d), F32), jax.ShapeDtypeStruct((vocab, d), F32)),
            in_specs=[pl.BlockSpec(memory_space=pl.ANY)] * 2,
            out_specs=(pl.BlockSpec(memory_space=pl.ANY), pl.BlockSpec(memory_space=pl.ANY)),
            scratch_shapes=[vmem((CHUNKS, d, tc), F32), vmem((tb, d), F32), vmem((vocab, d), F32), dma((8 + CHUNKS,)), dma((8 + CHUNKS,))],
        )(dht, dw)
        return loss[0, :1] * scale, dh, dw

    return jax.shard_map(local_head, mesh=mesh, in_specs=(tok_spec, P(("dp", "fsdp")), P("fsdp", None)), out_specs=(P("dp"), tok_spec, tok_spec), check_vma=False)
```
